32 devices in a mesh: section: 4 (over x, core), dp: 8 (over z, y).
Axes of the slice: x: 2, y: 2, z: 4, core: 2. Of those that a mesh axis runs over, the one named last changes fastest.
Arguments:
- clean_latent: float32 [64, 256], P('dp'), may hold values from -6 to 6
- noise_draw: float32 [64, 256], P('dp'), may hold values from -6 to 6
- step_index: int32 [64], P('dp'), may hold values from 250 to 1000
- labels: int32 [64], P('dp'), may hold values from 0 to 999
- guide_level: int32 [64], P('dp'), may hold values from 0 to 8
- class_table: bfloat16 [1001, 1152], replicated, may hold values from -6 to 6
- embed_in: bfloat16 [16, 1152], replicated, may hold values from -1.5 to 1.5
- embed_out: bfloat16 [1152, 16], replicated, may hold values from -0.1875 to 0.1875
- teacher_up: bfloat16 [4, 1152, 2304], P('section', 'dp'), may hold values from -0.1875 to 0.1875
- teacher_down: bfloat16 [4, 2304, 1152], P('section', 'dp'), may hold values from -0.125 to 0.125
- teacher_gain: float32 [4, 3, 1152], P('section'), may hold values from -3 to 3
- teacher_bias: float32 [4, 3, 1152], P('section'), may hold values from -3 to 3
- student_up: bfloat16 [1152, 4608], P(None, 'section'), may hold values from -0.1875 to 0.1875
- student_down: bfloat16 [4608, 1152], P('section'), may hold values from -0.09375 to 0.09375
- student_gain: float32 [3, 1152], replicated, may hold values from -3 to 3
- student_bias: float32 [3, 1152], replicated, may hold values from -3 to 3
- guide_vec: float32 [1152], replicated, may hold values from -3 to 3
Outputs:
- distill_target: float32 [64, 256], P('dp')
- grad_up: float32 [1152, 4608], P('dp', 'section')
- grad_down: float32 [4608, 1152], P(('section', 'dp'))
The draws below stay inside these ranges and needn't reach their ends.
All inputs are finite; a program needn't handle non-finite values.
Results may differ from the reference program's by a relative error of at most 0.017.
Values may be sent and summed in bfloat16 or wider, within the bound.
A program may use at most 128 MiB of HBM per device.

```python
import math
import jax
import jax.numpy as jnp
from jax import lax

D = 1152
FF_T = 2304
FF_S = 4608
CLASSES = 1000
CH = 16
TSTEPS = 1000
STRIDE = 125
SEQ = 16
SECTIONS = 4
SAMPLES = 64


def place_ends(entries, rng, least, largest):
    extent = entries.shape
    place = [jax.random.randint(jax.random.fold_in(rng, axis), (), 0, extent[axis]) for axis in range(len(extent))]
    entries = entries.at[tuple(place)].set(least)
    longest = extent.index(max(extent))
    place[longest] = (place[longest] + 1) % extent[longest]
    return entries.at[tuple(place)].set(largest)


def shard_levels(key, shape, pieces, smallest, high):
    factor_of, own = 1.0, jax.random.fold_in(key, 6)
    for axis_at, blocks in pieces:
        steps = jnp.exp(jax.random.uniform(jax.random.fold_in(own, axis_at), (blocks,), jnp.float32, smallest / len(pieces), high / len(pieces)))
        factor_of = factor_of * jnp.repeat(steps, shape[axis_at] // blocks).reshape([-1 if axis == axis_at else 1 for axis in range(len(shape))])
    return factor_of


def gaussian(own_key, shape, scale, reach, shards=(), held_as=jnp.bfloat16):
    entries = jax.random.normal(own_key, shape, jnp.float32) * scale
    if len(shards) > 0:
        entries = shard_levels(own_key, shape, shards, -0.22, 0.18) * entries
    return jnp.clip(entries, min=-reach, max=reach).astype(held_as)


def setup_inputs(seed: int = 0) -> dict:
    seeds = jax.random.split(jax.random.key(seed), 18)
    return {
        "clean_latent": gaussian(seeds[0], (SAMPLES, SEQ * CH), 1.0, 6.0, ((0, 8),), jnp.float32),
        "noise_draw": gaussian(seeds[1], (SAMPLES, SEQ * CH), 1.0, 6.0, ((0, 8),), jnp.float32),
        "step_index": place_ends(jax.random.randint(seeds[2], (SAMPLES,), 2 * STRIDE, TSTEPS + 1), jax.random.fold_in(seeds[2], 1), 2 * STRIDE, TSTEPS).astype(jnp.int32),
        "labels": place_ends(jax.random.randint(seeds[3], (SAMPLES,), 0, CLASSES), jax.random.fold_in(seeds[3], 1), 0, CLASSES - 1).astype(jnp.int32),
        "guide_level": place_ends(jax.random.randint(seeds[4], (SAMPLES,), 0, 9), jax.random.fold_in(seeds[4], 1), 0, 8).astype(jnp.int32),
        "class_table": gaussian(seeds[5], (CLASSES + 1, D), 1.0, 6.0),
        "embed_in": gaussian(seeds[6], (CH, D), CH ** -0.5, 1.5),
        "embed_out": gaussian(seeds[7], (D, CH), D ** -0.5, 0.1875),
        "teacher_up": gaussian(seeds[8], (SECTIONS, D, FF_T), D ** -0.5, 0.1875, ((0, 4), (1, 8))),
        "teacher_down": gaussian(seeds[9], (SECTIONS, FF_T, D), FF_T ** -0.5, 0.125, ((0, 4), (1, 8))),
        "teacher_gain": gaussian(seeds[10], (SECTIONS, 3, D), 0.5, 3.0, ((0, 4),), jnp.float32),
        "teacher_bias": gaussian(seeds[11], (SECTIONS, 3, D), 0.5, 3.0, ((0, 4),), jnp.float32),
        "student_up": gaussian(seeds[12], (D, FF_S), D ** -0.5, 0.1875, ((1, 4),)),
        "student_down": gaussian(seeds[13], (FF_S, D), FF_S ** -0.5, 0.09375, ((0, 4),)),
        "student_gain": gaussian(seeds[14], (3, D), 0.5, 3.0, (), jnp.float32),
        "student_bias": gaussian(seeds[15], (3, D), 0.5, 3.0, (), jnp.float32),
        "guide_vec": gaussian(seeds[16], (D,), 0.5, 3.0, (), jnp.float32),
    }


norm_eps = 1e-06

def layer_norm(values):
    center = values - lax.optimization_barrier(jnp.mean(values, axis=-1, keepdims=True))
    spread = lax.optimization_barrier(jnp.mean(center * center, axis=-1, keepdims=True))
    return center * lax.rsqrt(spread + norm_eps)

def sinusoid(step_ids, model_width):
    half_width = model_width // 2
    frequency = jnp.exp(-math.log(10000.0) * jnp.arange(half_width, dtype=jnp.float32) / half_width)
    phase_arg = step_ids.astype(jnp.float32)[:, None] * frequency[None, :]
    return jnp.concatenate([jnp.cos(phase_arg), jnp.sin(phase_arg)], axis=-1)

def plan(step_ids):
    angle_t = 0.5 * math.pi / TSTEPS * step_ids.astype(jnp.float32)
    return (jnp.cos(angle_t), jnp.sin(angle_t))

def embed_tokens(latent, embed_in):
    leading = latent.shape[0]
    patches = latent.reshape(leading * (latent.shape[1] // CH), CH).astype(jnp.bfloat16)
    tokens = jnp.dot(patches, embed_in, preferred_element_type=jnp.float32)
    return tokens.reshape(leading, latent.shape[1] // CH, embed_in.shape[1]).astype(jnp.bfloat16)

def mlp_block(inputs, modulation, up_proj, down_proj):
    groups, seq_len, model_width = inputs.shape
    residual_in = inputs.astype(jnp.float32)
    shift_rows = modulation[:, 0, None, :]
    scale_rows = modulation[:, 1, None, :]
    gate_rows = modulation[:, 2, None, :]
    normed = (layer_norm(residual_in) * (1.0 + scale_rows) + shift_rows).astype(jnp.bfloat16)
    pre_act = jnp.dot(normed.reshape(groups * seq_len, model_width), up_proj, preferred_element_type=jnp.float32)
    hidden = jax.nn.gelu(pre_act, approximate=True).astype(jnp.bfloat16)
    mixed = jnp.dot(hidden, down_proj, preferred_element_type=jnp.float32).reshape(groups, seq_len, model_width)
    return (residual_in + gate_rows * mixed).astype(jnp.bfloat16)

def velocity(states, embed_out):
    groups, seq_len, model_width = states.shape
    normed = layer_norm(states.astype(jnp.float32)).astype(jnp.bfloat16)
    result = jnp.dot(normed.reshape(groups * seq_len, model_width), embed_out, preferred_element_type=jnp.float32)
    return result.reshape(groups, seq_len * embed_out.shape[1])

def ddim_step(latent, predicted, time_now, time_next):
    alpha_now, sigma_now = plan(time_now)
    alpha_next, sigma_next = plan(time_next)
    clean_est = alpha_now[:, None] * latent - sigma_now[:, None] * predicted
    noise_est = sigma_now[:, None] * latent + alpha_now[:, None] * predicted
    return alpha_next[:, None] * clean_est + sigma_next[:, None] * noise_est

def gelu_slope(pre_act):
    return jax.vjp(lambda inner: jax.nn.gelu(inner, approximate=True), pre_act)[1](jnp.ones_like(pre_act))[0]

def reference(clean_latent, noise_draw, step_index, labels, guide_level, class_table, embed_in, embed_out, teacher_up, teacher_down, teacher_gain, teacher_bias, student_up, student_down, student_gain, student_bias, guide_vec):
    model_width = class_table.shape[1]
    samples = clean_latent.shape[0]
    seq_len = clean_latent.shape[1] // CH
    alpha_t, sigma_t = plan(step_index)
    noised = alpha_t[:, None] * clean_latent + sigma_t[:, None] * noise_draw
    guidance = 0.5 * guide_level.astype(jnp.float32)
    label_rows = jnp.take(class_table, labels, axis=0).astype(jnp.float32)
    null_row = class_table[class_table.shape[0] - 1].astype(jnp.float32)
    first_in = embed_tokens(noised, embed_in)
    latent = noised
    for which_step in range(2):
        time_now = step_index - which_step * STRIDE
        wave_rows = sinusoid(time_now, model_width)
        conditions = jnp.stack([wave_rows + label_rows, wave_rows + null_row[None, :]], axis=1)
        entry_rows = first_in if which_step == 0 else embed_tokens(latent, embed_in)
        states = jnp.stack([entry_rows, entry_rows], axis=1).reshape(samples * 2, seq_len, model_width)
        for layer in range(SECTIONS):
            modulation = conditions[:, :, None, :] * teacher_gain[layer] + teacher_bias[layer]
            states = mlp_block(states, modulation.reshape(samples * 2, 3, model_width), teacher_up[layer], teacher_down[layer])
        predicted = velocity(states, embed_out).reshape(samples, 2, seq_len * CH)
        guided = (1.0 + guidance)[:, None] * predicted[:, 0] - guidance[:, None] * predicted[:, 1]
        latent = ddim_step(latent, guided, time_now, time_now - STRIDE)
    alpha_end, sigma_end = plan(step_index - 2 * STRIDE)
    sigma_ratio = sigma_end / sigma_t
    distill_target = (latent - sigma_ratio[:, None] * noised) / (alpha_end - sigma_ratio * alpha_t)[:, None]
    student_cond = sinusoid(step_index, model_width) + label_rows + guidance[:, None] * guide_vec[None, :]
    modulation = student_cond[:, None, :] * student_gain[None] + student_bias[None]
    shift_rows = modulation[:, 0, None, :]
    scale_rows = modulation[:, 1, None, :]
    gate_rows = modulation[:, 2, None, :]
    row_count = samples * seq_len
    residual_in = first_in.astype(jnp.float32)
    normed = (layer_norm(residual_in) * (1.0 + scale_rows) + shift_rows).astype(jnp.bfloat16).reshape(row_count, model_width)
    pre_act = jnp.dot(normed, student_up, preferred_element_type=jnp.float32)
    hidden = jax.nn.gelu(pre_act, approximate=True).astype(jnp.bfloat16)
    mixed = jnp.dot(hidden, student_down, preferred_element_type=jnp.float32).reshape(samples, seq_len, model_width)
    state_rows = residual_in + gate_rows * mixed
    normed_out, pullback = jax.vjp(layer_norm, state_rows)
    predicted = jnp.dot(normed_out.astype(jnp.bfloat16).reshape(row_count, model_width), embed_out, preferred_element_type=jnp.float32).reshape(samples, seq_len * CH)
    estimate = alpha_t[:, None] * noised - sigma_t[:, None] * predicted
    weight = jnp.maximum(alpha_t * alpha_t / (sigma_t * sigma_t), 1.0)
    element_count = clean_latent.shape[0] * clean_latent.shape[1]
    slope_pred = -2.0 / element_count * (sigma_t * weight)[:, None] * (estimate - distill_target)
    back_norm = jnp.dot(slope_pred.reshape(row_count, CH), embed_out.astype(jnp.float32).T, precision=lax.Precision.HIGHEST)
    back_state = pullback(back_norm.reshape(samples, seq_len, model_width))[0]
    back_part = (gate_rows * back_state).astype(jnp.bfloat16).reshape(row_count, model_width)
    back_hidden = lax.dot_general(back_part, student_down, (((1,), (1,)), ((), ())), preferred_element_type=jnp.float32)
    back_pre = (back_hidden * gelu_slope(pre_act)).astype(jnp.bfloat16)
    grad_up = lax.dot_general(normed, back_pre, (((0,), (0,)), ((), ())), preferred_element_type=jnp.float32)
    grad_down = lax.dot_general(hidden, back_part, (((0,), (0,)), ((), ())), preferred_element_type=jnp.float32)
    return (distill_target, grad_up, grad_down)
```

```python
import functools
import math

import jax
import jax.numpy as jnp
import numpy as np
from jax import lax
from jax.experimental import pallas as pl
from jax.experimental.pallas import tpu as pltpu
from jax.sharding import PartitionSpec as P

CH = 16
TSTEPS = 1000
STRIDE = 125


norm_eps = 1e-06


def shifted(shard, axis, by):
    length = lax.axis_size(axis)
    return lax.ppermute(shard, axis, [(i, (i + by) % length) for i in range(length)])


def from_root(shard, axis, root):
    mine = lax.axis_index(axis) == root
    return lax.psum(jnp.where(mine, shard, jnp.zeros_like(shard)), axis)


def layer_norm(values):
    center = values - jnp.mean(values, axis=-1, keepdims=True)
    spread = jnp.mean(center * center, axis=-1, keepdims=True)
    return center * lax.rsqrt(spread + norm_eps)


def sinusoid(step_ids, model_width):
    half_width = model_width // 2
    frequency = jnp.exp(-math.log(10000.0) * jnp.arange(half_width, dtype=jnp.float32) / half_width)
    phase_arg = step_ids.astype(jnp.float32)[:, None] * frequency[None, :]
    return jnp.concatenate([jnp.cos(phase_arg), jnp.sin(phase_arg)], axis=-1)


def plan(step_ids):
    angle_t = 0.5 * math.pi / TSTEPS * step_ids.astype(jnp.float32)
    return (jnp.cos(angle_t), jnp.sin(angle_t))


def embed_tokens(latent, embed_in):
    leading = latent.shape[0]
    patches = latent.reshape(leading * (latent.shape[1] // CH), CH).astype(jnp.bfloat16)
    tokens = jnp.dot(patches, embed_in, preferred_element_type=jnp.float32)
    return tokens.reshape(leading, latent.shape[1] // CH, embed_in.shape[1]).astype(jnp.bfloat16)


def mlp_block(inputs, modulation, up_proj, down_proj):
    groups, seq_len, model_width = inputs.shape
    residual_in = inputs.astype(jnp.float32)
    shift_rows = modulation[:, 0, None, :]
    scale_rows = modulation[:, 1, None, :]
    gate_rows = modulation[:, 2, None, :]
    normed = (layer_norm(residual_in) * (1.0 + scale_rows) + shift_rows).astype(jnp.bfloat16)
    pre_act = jnp.dot(
        normed.reshape(groups * seq_len, model_width), up_proj, preferred_element_type=jnp.float32
    )
    hidden = jax.nn.gelu(pre_act, approximate=True).astype(jnp.bfloat16)
    mixed = jnp.dot(hidden, down_proj, preferred_element_type=jnp.float32).reshape(
        groups, seq_len, model_width
    )
    return (residual_in + gate_rows * mixed).astype(jnp.bfloat16)


def velocity(states, embed_out):
    groups, seq_len, model_width = states.shape
    normed = layer_norm(states.astype(jnp.float32)).astype(jnp.bfloat16)
    result = jnp.dot(
        normed.reshape(groups * seq_len, model_width), embed_out, preferred_element_type=jnp.float32
    )
    return result.reshape(groups, seq_len * embed_out.shape[1])


def ddim_step(latent, predicted, time_now, time_next):
    alpha_now, sigma_now = plan(time_now)
    alpha_next, sigma_next = plan(time_next)
    clean_est = alpha_now[:, None] * latent - sigma_now[:, None] * predicted
    noise_est = sigma_now[:, None] * latent + alpha_now[:, None] * predicted
    return alpha_next[:, None] * clean_est + sigma_next[:, None] * noise_est


def gelu_slope(pre_act):
    return jax.vjp(lambda inner: jax.nn.gelu(inner, approximate=True), pre_act)[1](
        jnp.ones_like(pre_act)
    )[0]


def run_chunks(count, one, operands, shared):
    if count == 1:
        return one(operands, *shared)

    def step(carry, piece):
        out = one(piece, *shared)
        return (carry[0] + out[0], carry[1] + out[1]), None

    split = [a.reshape((count, a.shape[0] // count) + a.shape[1:]) for a in operands]
    shapes = jax.eval_shape(one, [a[0] for a in split], *shared)
    zeros = tuple(jnp.zeros(s.shape, s.dtype) for s in shapes)
    return lax.scan(step, zeros, split)[0]


def teacher_chain(first_in, noised, guidance, step_index, mods, up, down, embed_in, embed_out):
    section_count = lax.axis_size("section")
    section_at = lax.axis_index("section")
    micro, seq_len, model_width = first_in.shape

    def paired(tokens):
        return jnp.broadcast_to(tokens[:, None], (micro, 2, seq_len, model_width)).reshape(
            2 * micro, seq_len, model_width
        )

    latent = noised
    states = paired(first_in)
    for which_step in range(2):
        mod = mods[which_step].reshape(2 * micro, 3, model_width)
        if which_step:
            states = paired(embed_tokens(latent, embed_in))
        for layer in range(section_count):
            states = mlp_block(states, mod, up, down)
            if layer < section_count - 1:
                states = lax.ppermute(states, "section", [(layer, layer + 1)])
        predicted = velocity(states, embed_out).reshape(micro, 2, -1)
        weight = guidance[:, None]
        guided = (1.0 + weight) * predicted[:, 0] - weight * predicted[:, 1]
        time_now = step_index - which_step * STRIDE
        stepped = ddim_step(latent, guided, time_now, time_now - STRIDE)
        if which_step == 0:
            returned = lax.ppermute(
                stepped, "section", [(section_count - 1, 0)]
            )
            latent = jnp.where(section_at == section_count - 1, stepped, returned)
    return stepped


def cos_of(angle, shift_quarter):
    quarters = jnp.floor(angle * (2.0 / math.pi) + 0.5)
    rest = ((angle - quarters * 1.5703125) - quarters * 4.837512969970703125e-4) - (
        quarters * 7.549789954891882e-8
    )
    turn = quarters - shift_quarter
    turn = turn - 4.0 * jnp.floor(turn * 0.25)
    square = rest * rest
    sine = rest + rest * square * (
        -1.6666654611e-1 + square * (8.3321608736e-3 - 1.9515295891e-4 * square)
    )
    cosine = (
        1.0
        - 0.5 * square
        + square
        * square
        * (4.166664568298827e-2 + square * (-1.388731625493765e-3 + 2.443315711809948e-5 * square))
    )
    odd = (turn == 1.0) | (turn == 3.0)
    negative = (turn == 1.0) | (turn == 2.0)
    value = jnp.where(odd, sine, cosine)
    return jnp.where(negative, -value, value)


NT = (((1,), (1,)), ((), ()))
GELU_A = math.sqrt(2.0 / math.pi)
GELU_B = 0.044715


def dot32(a, b, dims=(((1,), (0,)), ((), ()))):
    return lax.dot_general(a, b, dims, preferred_element_type=jnp.float32)


def gelu_pair(pre):
    square = pre * pre
    bent = jnp.tanh(GELU_A * (pre + GELU_B * square * pre))
    half = 0.5 * (1.0 + bent)
    slope = half + 0.5 * pre * (1.0 - bent * bent) * (GELU_A * (1.0 + 3.0 * GELU_B * square))
    return pre * half, slope


def token_mask(first, count, shape):
    lane = lax.broadcasted_iota(jnp.int32, shape, 1) // CH
    return [lane == first + k for k in range(count)]


def spread(values, first, count):
    masks = token_mask(first, count, values.shape)
    zero = jnp.zeros_like(values)
    return jnp.concatenate([jnp.where(m, values, zero) for m in masks], axis=0)


def gathered_tokens(values, first, count, rows):
    masks = token_mask(first, count, (rows, values.shape[1]))
    total = jnp.zeros((rows, values.shape[1]), jnp.float32)
    for k in range(count):
        total = total + jnp.where(masks[k], values[k * rows : (k + 1) * rows], 0.0)
    return total


def mega_kernel(
    dims,
    steps_in, labels_in, levels_in, clean_in, noise_in, up_shard, down_shard, t_gain, t_bias, s_gain, s_bias, guide_vec, freq,
    embed_in, embed_out_t, stud_up_hbm, stud_down_hbm, table_hbm,
    target_out, grad_up, grad_down,
    stud_up, stud_down, table, packed, up, down, tiled_in, tiled_out,
    noised, cols, wave, labs, scond, tok, slope, n_share, h_share, parts, pair_in, pair_sum,
    cross_in, mixed, xhat, rstd, pred, states, outs, latents, velo, target_all, hid,
    local_sem, send, recv, move_send, move_recv, z_send, z_recv, t_send, t_recv,
):
    sections, dps, micro, seq_len = dims
    total = dps * micro
    width = clean_in.shape[1]
    model = embed_in.shape[1]
    sec = lax.axis_index("section")
    me = lax.axis_index("dp")
    z, y = me // 2, me % 2
    core, side = sec % 2, z // 2
    tail = sections - 1
    mid_z, end_z, far_mid_z = 1 + side, 3 * side, 2 - side
    far_end_z = 3 - end_z
    is_mid = z == mid_z
    is_end = z == end_z
    oy = 1 - y
    E_y, E_o = end_z * 2 + y, end_z * 2 + oy
    A_y, A_o = mid_z * 2 + y, mid_z * 2 + oy
    B_y, B_o = far_mid_z * 2 + y, far_mid_z * 2 + oy
    F_y, F_o = far_end_z * 2 + y, far_end_z * 2 + oy
    MESH = pl.DeviceIdType.MESH
    devices = sections * dps
    mine = sec * dps + me

    barrier = pltpu.get_barrier_semaphore()

    def greet(k, carry):
        other = lax.rem(mine + k, devices)
        pl.semaphore_signal(
            barrier, inc=1, device_id={"section": other // dps, "dp": lax.rem(other, dps)},
            device_id_type=MESH,
        )
        return carry

    def place(who):
        zz, yy = who // 2, who % 2
        return (zz % 2) * (dps // 2) + (zz // 2) * 2 + yy

    lax.fori_loop(1, devices, greet, 0)
    row = lax.broadcasted_iota(jnp.int32, (micro, 128), 0)
    column = lax.broadcasted_iota(jnp.int32, (micro, 128), 1)
    cells = jnp.zeros((micro, 128), jnp.float32)
    for k, ref in enumerate((steps_in, labels_in, levels_in)):
        for b in range(micro):
            cells = jnp.where((row == b) & (column == k), ref[b].astype(jnp.float32), cells)
    slot = place(me)
    packed[slot, :, 0:width] = clean_in[...]
    packed[slot, :, width : 2 * width] = noise_in[...]
    packed[slot, :, 2 * width :] = cells
    locals_ = [
        pltpu.make_async_copy(stud_up_hbm, stud_up, local_sem.at[0]),
        pltpu.make_async_copy(stud_down_hbm, stud_down, local_sem.at[1]),
        pltpu.make_async_copy(table_hbm, table, local_sem.at[2]),
    ]
    for c in locals_:
        c.start()
    pl.semaphore_wait(barrier, devices - 1)

    def copy(i, src, dst, **device):
        return pltpu.make_async_remote_copy(
            src_ref=src, dst_ref=dst, send_sem=send.at[i], recv_sem=recv.at[i],
            device_id=device, device_id_type=MESH,
        )

    ur, dr = up_shard.shape[0], down_shard.shape[0]

    def urow(who):
        return up.at[pl.ds(pl.multiple_of(who * ur, 16), ur)]

    def drow(who, lo=0, n=None):
        return down.at[pl.ds(pl.multiple_of(who * dr + lo, 16), dr if n is None else n)]

    packs = [
        copy(k - 1, packed.at[slot], packed.at[slot], dp=lax.rem(me + k, dps))
        for k in range(1, dps)
    ]
    for c in packs:
        c.start()
    base = dps - 1
    names = [
        "ey_u", "ey_d", "ez_u", "ez_d", "ezo_u", "ezo_d", "det1", "det2", "det3",
        "ay_u", "ay_d", "am_u", "am_d", "ame_u", "ame_d", "amo",
        "ayf_u", "ayf_d", "aye_u", "aye_d", "pair", "cross", "back",
    ]
    index = {n: base + k for k, n in enumerate(names)}
    cut = (2 * dr // 3) // 16 * 16
    low, high = (0, cut), (cut, dr - cut)
    span = {"det1": low, "det2": low, "det3": low, "amo": low, "ay_d": high, "aye_d": high}

    def own(name, dst):
        if name.endswith("u"):
            return copy(index[name], up_shard, urow(me), dp=dst)
        lo, n = span.get(name, (0, dr))
        return copy(index[name], down_shard.at[pl.ds(lo, n)], drow(me, lo, n), dp=dst)

    def piece(name, who, dst):
        ref = urow(who) if name.endswith("u") else drow(who, *span.get(name, (0, dr)))
        return copy(index[name], ref, ref, dp=dst)

    end_sends = (("ez_u", A_y), ("ey_u", E_o), ("ez_d", A_y), ("ey_d", E_o))
    mid_sends = (
        ("am_u", B_y), ("ay_u", A_o), ("det1", E_y), ("am_d", B_y), ("ay_d", A_o)
    )

    @pl.when(is_end)
    def _():
        for n, dst in end_sends:
            own(n, dst).start()

    @pl.when(is_mid)
    def _():
        for n, dst in mid_sends:
            own(n, dst).start()
        up[pl.ds(pl.multiple_of(me * ur, 16), ur)] = up_shard[...]
        down[pl.ds(pl.multiple_of(me * dr, 16), dr)] = down_shard[...]

    def relay(part):
        @pl.when(is_end)
        def _():
            piece("ey_" + part, E_o, E_o).wait_recv()
            piece("ezo_" + part, E_o, A_y).start()
            if part == "u":
                piece("det1", A_y, E_o).wait_recv()
                piece("det2", A_y, E_o).start()
            else:
                piece("det2", A_o, A_y).wait_recv()
                piece("det3", A_o, A_y).start()

        @pl.when(is_mid)
        def _():
            piece("ez_" + part, E_y, B_y).wait_recv()
            piece("ame_" + part, E_y, B_y).start()
            piece("am_" + part, B_y, A_o).wait_recv()
            piece("ayf_" + part, B_y, A_o).start()

    for k in range(seq_len):
        tiled_in[k * CH : (k + 1) * CH] = embed_in[...]
        tiled_out[k * CH : (k + 1) * CH] = embed_out_t[...]
    lane_model = lax.broadcasted_iota(jnp.int32, (1, model), 1)
    sine_lane = jnp.where(lane_model >= model // 2, 1.0, 0.0)
    for c in packs:
        c.wait_recv()
    data = packed[...].reshape(total, packed.shape[2])
    steps = data[:, 2 * width : 2 * width + 1]
    label = data[:, 2 * width + 1 : 2 * width + 2]
    guide = 0.5 * data[:, 2 * width + 2 : 2 * width + 3]
    for k in range(3):
        angle = jnp.broadcast_to(
            (0.5 * math.pi / TSTEPS) * (steps - float(k * STRIDE)), (total, 128)
        )
        cols[2 * k] = cos_of(angle, 0.0)
        cols[2 * k + 1] = cos_of(angle, 1.0)
    cols[6] = jnp.broadcast_to(guide, (total, 128))
    alpha_t, sigma_t = cols[0][:, 0:1], cols[1][:, 0:1]
    clean = alpha_t * data[:, :width] + sigma_t * data[:, width : 2 * width]
    noised[...] = clean
    for k in range(2):
        wave[k] = cos_of((steps - float(k * STRIDE)) * freq[...], sine_lane)
    for c in locals_:
        c.wait()
    classes = table.shape[0] - 1
    whole = (classes // 16) * 16
    ids = lax.broadcasted_iota(jnp.int32, (total, whole), 1).astype(jnp.float32)
    rows = dot32(jnp.where(ids == label, 1.0, 0.0).astype(jnp.bfloat16), table[:whole])
    rest = table[whole:].astype(jnp.float32)
    for k in range(classes - whole):
        rows = rows + jnp.where(label == float(whole + k), rest[k : k + 1], 0.0)
    labs[0] = rows
    labs[1] = jnp.broadcast_to(rest[classes - whole : classes - whole + 1], (total, model))
    scond[...] = wave[0] + rows + guide * guide_vec[...]

    block = seq_len // 2
    blocks = 4
    group = total // 2
    brows = block * group
    share = n_share.shape[0]
    pick = jnp.where(
        lax.broadcasted_iota(jnp.int32, (share, model), 1)
        == lax.broadcasted_iota(jnp.int32, (share, model), 0) + me * share,
        1.0, 0.0,
    ).astype(jnp.bfloat16)

    def at_block(i):
        return pl.ds(pl.multiple_of(i * brows, brows), brows)

    def members(i):
        return pl.ds(pl.multiple_of((i // 2) * group, group), group)

    def first_of(i):
        return lax.rem(i, 2) * block

    def student_part(i, k):
        return scond[members(i)] * s_gain[k : k + 1] + s_bias[k : k + 1]

    def front(i, carry):
        here = at_block(i)
        tokens = dot32(
            spread(noised[members(i)], first_of(i), block).astype(jnp.bfloat16), tiled_in[...]
        ).astype(jnp.bfloat16)
        tok[here] = tokens
        cube = layer_norm(tokens.astype(jnp.float32)).reshape(block, group, model)
        normed = (cube * (1.0 + student_part(i, 1))[None] + student_part(i, 0)[None]).astype(
            jnp.bfloat16
        )
        normed = normed.reshape(brows, model)
        n_share[:, here] = dot32(pick, normed, NT).astype(jnp.bfloat16)
        hidden, bend = gelu_pair(dot32(normed, stud_up[...]))
        hidden = hidden.astype(jnp.bfloat16)
        slope[here] = bend
        h_share[:, here] = dot32(pick, hidden, NT).astype(jnp.bfloat16)
        parts[here] = dot32(hidden, stud_down[...]).astype(jnp.bfloat16)
        return carry

    lax.fori_loop(0, blocks, front, 0)

    half_rows = seq_len * total // 2

    def half_of(ref, c):
        return ref.at[pl.ds(pl.multiple_of(c * half_rows, half_rows), half_rows)]

    sibling = sec + 1 - 2 * core
    pair = copy(index["pair"], half_of(parts, 1 - core), pair_in, section=sibling)
    cross = copy(index["cross"], pair_sum, cross_in, section=lax.rem(sec + 2, sections))
    back = copy(index["back"], half_of(mixed, core), half_of(mixed, core), section=sibling)
    pair.start()
    relay("u")
    pair.wait_recv()
    pair_sum[...] = (
        half_of(parts, core)[...].astype(jnp.float32) + pair_in[...].astype(jnp.float32)
    ).astype(jnp.bfloat16)
    cross.start()
    relay("d")
    turned = model // 4

    def turn(i, carry):
        here = pl.ds(pl.multiple_of(i * turned, turned), turned)
        eye = jnp.where(
            lax.broadcasted_iota(jnp.int32, (turned, model), 1)
            == lax.broadcasted_iota(jnp.int32, (turned, model), 0) + i * turned,
            1.0, 0.0,
        ).astype(jnp.bfloat16)
        stud_up[here] = dot32(eye, stud_down[...], NT).astype(jnp.bfloat16)
        return carry

    lax.fori_loop(0, 4, turn, 0)

    @pl.when(is_mid)
    def _():
        piece("ame_u", F_y, A_o).wait_recv()
        piece("aye_u", F_y, A_o).start()

    cross.wait_recv()
    mixed[pl.ds(pl.multiple_of(core * half_rows, half_rows), half_rows)] = (
        pair_sum[...].astype(jnp.float32) + cross_in[...].astype(jnp.float32)
    ).astype(jnp.bfloat16)
    back.start()

    @pl.when(is_mid)
    def _():
        piece("ezo_d", E_o, B_y).wait_recv()
        piece("amo", E_o, B_y).start()
        piece("ame_d", F_y, A_o).wait_recv()
        piece("aye_d", F_y, A_o).start()

    back.wait_recv()
    pred[...] = jnp.zeros_like(pred)

    def middle(i, carry):
        here = at_block(i)
        state = tok[here].astype(jnp.float32).reshape(block, group, model) + student_part(i, 2)[
            None
        ] * mixed[here].astype(jnp.float32).reshape(block, group, model)
        state = state.reshape(brows, model)
        center = state - jnp.mean(state, axis=-1, keepdims=True)
        inverse = lax.rsqrt(jnp.mean(center * center, axis=-1, keepdims=True) + norm_eps)
        unit = center * inverse
        xhat[here] = unit
        rstd[here] = jnp.broadcast_to(inverse, (brows, 128))
        pred[members(i)] += gathered_tokens(
            dot32(unit.astype(jnp.bfloat16), tiled_out[...], NT), first_of(i), block, group
        )
        return carry

    lax.fori_loop(0, blocks, middle, 0)

    trows = micro * seq_len
    chunk = 768 if up.shape[1] % 768 == 0 else up.shape[1]

    def owned(j):
        return j * (dps // 2) + (z - 1) * 2 + y

    def sample_rows(d):
        return pl.ds(pl.multiple_of(d * micro, micro), micro)

    def move(i):
        return pltpu.make_async_remote_copy(
            src_ref=outs.at[i], dst_ref=states.at[i],
            send_sem=move_send.at[i], recv_sem=move_recv.at[i],
            device_id={"section": lax.rem(sec + 1, sections)}, device_id_type=MESH,
        )

    def back_move(j):
        return pltpu.make_async_remote_copy(
            src_ref=latents.at[1, j], dst_ref=latents.at[1, j],
            send_sem=z_send.at[j], recv_sem=z_recv.at[j],
            device_id={"section": 0}, device_id_type=MESH,
        )

    def target_copy(k, j, d):
        other = lax.rem(mine + k, devices)
        return pltpu.make_async_remote_copy(
            src_ref=target_all.at[d], dst_ref=target_all.at[d],
            send_sem=t_send.at[j * devices + k], recv_sem=t_recv.at[d],
            device_id={"section": other // dps, "dp": lax.rem(other, dps)}, device_id_type=MESH,
        )

    @pl.when(is_mid)
    def _():
        for n, who in (
            ("ay_u", A_o), ("ay_d", A_o), ("det3", A_o), ("ayf_u", B_o), ("ayf_d", B_o),
            ("ezo_u", E_o), ("aye_u", F_o), ("aye_d", F_o), ("amo", F_o),
        ):
            piece(n, who, A_o).wait_recv()
        for j in range(2):
            latents[0, j] = noised[sample_rows(owned(j))]

        def task(i, carry):
            step, j, half = i // 4, lax.rem(i // 2, 2), lax.rem(i, 2)
            d = owned(j)
            here = sample_rows(d)

            @pl.when(sec == 0)
            def _():
                @pl.when((step == 1) & (half == 0))
                def _():
                    back_move(j).wait_recv()

                states[i] = dot32(
                    spread(latents[step, j], 0, seq_len).astype(jnp.bfloat16), tiled_in[...]
                ).astype(jnp.bfloat16)

            @pl.when(sec > 0)
            def _():
                move(i).wait_recv()

            cond = wave[step, here] + labs[half, here]
            residual = states[i].astype(jnp.float32)
            cube = layer_norm(residual).reshape(seq_len, micro, model)
            scale = cond * t_gain[1] + t_bias[1]
            shift = cond * t_gain[0] + t_bias[0]
            gate = cond * t_gain[2] + t_bias[2]
            normed = (cube * (1.0 + scale)[None] + shift[None]).astype(jnp.bfloat16)
            normed = normed.reshape(trows, model)
            for k in range(up.shape[1] // chunk):
                hid[:, k * chunk : (k + 1) * chunk] = jax.nn.gelu(
                    dot32(normed, up[:, k * chunk : (k + 1) * chunk]), approximate=True
                ).astype(jnp.bfloat16)
            acc = dot32(hid[...], down[...])
            out = residual.reshape(seq_len, micro, model) + gate[None] * acc.reshape(
                seq_len, micro, model
            )
            outs[i] = out.reshape(trows, model).astype(jnp.bfloat16)

            @pl.when(sec < tail)
            def _():
                move(i).start()

            @pl.when(sec == tail)
            def _():
                last = layer_norm(outs[i].astype(jnp.float32)).astype(jnp.bfloat16)
                velo[half] = gathered_tokens(
                    dot32(last, tiled_out[...], NT), 0, seq_len, micro
                )

                @pl.when(half == 1)
                def _():
                    level = cols[6, here][:, 0:1]
                    guided = (1.0 + level) * velo[0] - level * velo[1]
                    a_now = cols[2 * step, here][:, 0:1]
                    s_now = cols[2 * step + 1, here][:, 0:1]
                    a_next = cols[2 * step + 2, here][:, 0:1]
                    s_next = cols[2 * step + 3, here][:, 0:1]
                    before = latents[step, j]
                    after = a_next * (a_now * before - s_now * guided) + s_next * (
                        s_now * before + a_now * guided
                    )

                    @pl.when(step == 0)
                    def _():
                        latents[1, j] = after
                        back_move(j).start()

                    @pl.when(step == 1)
                    def _():
                        a_first, s_first = cols[0, here][:, 0:1], cols[1, here][:, 0:1]
                        ratio = s_next / s_first
                        target_all[d] = (after - ratio * latents[0, j]) / (a_next - ratio * a_first)

                        def tell(k, carry):
                            target_copy(k, j, d).start()
                            return carry

                        lax.fori_loop(1, devices, tell, 0)

            return carry

        lax.fori_loop(0, 8, task, 0)

    grad_up[...] = jnp.zeros_like(grad_up)
    grad_down[...] = jnp.zeros_like(grad_down)

    def finish(i, carry):
        here = at_block(i)
        slopes = dot32(
            spread(pred[members(i)], first_of(i), block).astype(jnp.bfloat16), tiled_out[...]
        ) + dot32(
            spread(noised[members(i)], first_of(i), block).astype(jnp.bfloat16), tiled_out[...]
        )
        unit = xhat[here]
        mean = jnp.mean(slopes, axis=-1, keepdims=True)
        along = jnp.mean(slopes * unit, axis=-1, keepdims=True)
        back_state = rstd[here][:, 0:1] * (slopes - mean - unit * along)
        back_part = (student_part(i, 2)[None] * back_state.reshape(block, group, model)).astype(
            jnp.bfloat16
        ).reshape(brows, model)
        grad_down[...] += dot32(h_share[:, here], back_part)
        back_pre = (dot32(back_part, stud_up[...]) * slope[here]).astype(jnp.bfloat16)
        grad_up[...] += dot32(n_share[:, here], back_pre)
        return carry

    for part in range(2):
        for k in range(dps // 2):
            d = part * (dps // 2) + k

            @pl.when(jnp.logical_not((sec == tail) & (z == 1 + k // 2) & (y == k % 2)))
            def _():
                target_copy(1, 0, d).wait_recv()

        these = pl.ds(part * group, group)
        alpha_h, sigma_h = cols[0, these][:, 0:1], cols[1, these][:, 0:1]
        weight = jnp.maximum(alpha_h * alpha_h / (sigma_h * sigma_h), 1.0)
        estimate = alpha_h * noised[these] - sigma_h * pred[these]
        goal = target_all[pl.ds(part * (dps // 2), dps // 2)].reshape(group, width)
        seed = (-2.0 / (total * width)) * (sigma_h * weight) * (estimate - goal)
        seed_hi = seed.astype(jnp.bfloat16).astype(jnp.float32)
        pred[these] = seed_hi
        noised[these] = seed - seed_hi
        lax.fori_loop(2 * part, 2 * part + 2, finish, 0)

    target_out[...] = target_all[slot]

    for c in packs + [pair, cross, back]:
        c.wait_send()

    @pl.when(is_end)
    def _():
        for n, dst in end_sends:
            own(n, dst).wait_send()
        for n, who, dst in (
            ("ezo_u", E_o, A_y), ("ezo_d", E_o, A_y), ("det2", A_y, E_o), ("det3", A_o, A_y)
        ):
            piece(n, who, dst).wait_send()

    @pl.when(is_mid)
    def _():
        for n, dst in mid_sends:
            own(n, dst).wait_send()
        for n, who, dst in (
            ("ame_u", E_y, B_y), ("ame_d", E_y, B_y), ("amo", E_o, B_y),
            ("ayf_u", B_y, A_o), ("ayf_d", B_y, A_o), ("aye_u", F_y, A_o), ("aye_d", F_y, A_o),
        ):
            piece(n, who, dst).wait_send()

        @pl.when(sec < tail)
        def _():
            def done(i, carry):
                move(i).wait_send()
                return carry

            lax.fori_loop(0, 8, done, 0)

        @pl.when(sec == tail)
        def _():
            for j in range(2):
                back_move(j).wait_send()

                def told(k, carry):
                    target_copy(k, j, owned(j)).wait_send()
                    return carry

                lax.fori_loop(1, devices, told, 0)


def flush_kernel(a, b, c, x, y, z):
    x[...] = a[...]
    y[...] = b[...]
    z[...] = c[...]


def mega_call(dims, operands):
    sections, dps, micro, seq_len = dims
    clean, up_shard, down_shard = operands[3], operands[5], operands[6]
    hidden, model = up_shard.shape[1], down_shard.shape[1]
    stud_up, stud_down, table = operands[-3:]
    width = clean.shape[1]
    total = dps * micro
    rows = total * seq_len
    trows = micro * seq_len
    share_up, share_down = model // dps, stud_down.shape[0] // dps
    f32, bf16 = jnp.float32, jnp.bfloat16
    vmem = pl.BlockSpec(memory_space=pltpu.VMEM)
    hbm = pl.BlockSpec(memory_space=pl.ANY)
    smem = pl.BlockSpec(memory_space=pltpu.SMEM)
    V, D = pltpu.VMEM, pltpu.SemaphoreType.DMA
    results = pl.pallas_call(
        functools.partial(mega_kernel, dims),
        out_shape=(
            jax.ShapeDtypeStruct((micro, width), f32),
            jax.ShapeDtypeStruct((share_up, stud_up.shape[1]), f32),
            jax.ShapeDtypeStruct((share_down, model), f32),
        ),
        in_specs=[smem] * 3 + [vmem] * (len(operands) - 6) + [hbm] * 3,
        out_specs=(vmem,) * 3,
        scratch_shapes=[
            V(stud_up.shape, bf16), V(stud_down.shape, bf16), V(table.shape, bf16),
            V((dps, micro, 2 * width + 128), f32),
            V((up_shard.shape[0] * dps, hidden), bf16),
            V((down_shard.shape[0] * dps, model), bf16),
            V((width, model), bf16), V((width, model), bf16),
            V((total, width), f32), V((7, total, 128), f32),
            V((2, total, model), f32), V((2, total, model), f32), V((total, model), f32),
            V((rows, model), bf16), V((rows, model), f32),
            V((share_up, rows), bf16), V((share_down, rows), bf16),
            V((rows, model), bf16), V((rows // 2, model), bf16), V((rows // 2, model), bf16),
            V((rows // 2, model), bf16), V((rows, model), bf16),
            V((rows, model), f32), V((rows, 128), f32), V((total, width), f32),
            V((8, trows, model), bf16), V((8, trows, model), bf16),
            V((2, 2, micro, width), f32), V((2, micro, width), f32), V((dps, micro, width), f32),
            V((trows, hidden), bf16),
            D((3,)), D((32,)), D((32,)), D((8,)), D((8,)), D((2,)), D((2,)),
            D((2 * sections * dps,)), D((dps,)),
        ],
        compiler_params=pltpu.CompilerParams(
            collective_id=0, has_side_effects=True, vmem_limit_bytes=63 << 20
        ),
    )(*operands)
    return pl.pallas_call(
        flush_kernel,
        out_shape=tuple(jax.ShapeDtypeStruct(r.shape, r.dtype) for r in results),
        in_specs=[vmem] * 3,
        out_specs=(vmem,) * 3,
    )(*results)


def body(
    clean_latent,
    noise_draw,
    step_index,
    labels,
    guide_level,
    class_table,
    embed_in,
    embed_out,
    teacher_up,
    teacher_down,
    teacher_gain,
    teacher_bias,
    student_up,
    student_down,
    student_gain,
    student_bias,
    guide_vec,
):
    section_count = lax.axis_size("section")
    dp_count = lax.axis_size("dp")
    section_at = lax.axis_index("section")
    dp_at = lax.axis_index("dp")
    micro = clean_latent.shape[0]
    width = clean_latent.shape[1]
    seq_len = width // CH
    model_width = class_table.shape[1]
    fused = (
        dp_count == 8
        and section_count == 4
        and micro == 8
        and seq_len % 4 == 0
        and width % 128 == 0
        and teacher_up.shape[1] % 16 == 0
        and teacher_down.shape[1] % 16 == 0
        and student_up.shape[1] == student_down.shape[0] == model_width
    )
    if fused:
        half_width = model_width // 2
        frequency = np.exp(-math.log(10000.0) * np.arange(half_width) / half_width)
        frequency = np.tile(frequency, 2)[None].astype(np.float32)
        return mega_call(
            (section_count, dp_count, micro, seq_len),
            (
                step_index, labels, guide_level, clean_latent, noise_draw,
                teacher_up[0], teacher_down[0],
                teacher_gain.reshape(3, 1, model_width), teacher_bias.reshape(3, 1, model_width),
                student_gain, student_bias, guide_vec[None], jnp.asarray(frequency),
                embed_in, embed_out.T, student_up, student_down, class_table,
            ),
        )
    alpha_t, sigma_t = plan(step_index)
    noised = alpha_t[:, None] * clean_latent + sigma_t[:, None] * noise_draw
    guidance = 0.5 * guide_level.astype(jnp.float32)
    label_rows = jnp.take(class_table, labels, axis=0).astype(jnp.float32)
    null_row = class_table[class_table.shape[0] - 1].astype(jnp.float32)
    wave_rows = jnp.stack(
        [sinusoid(step_index - step_k * STRIDE, model_width) for step_k in range(2)]
    )
    conditions = jnp.stack(
        [wave_rows + label_rows[None], wave_rows + null_row[None, None, :]], axis=2
    )
    mods = (
        conditions[:, :, :, None, :] * teacher_gain[0][None, None, None]
        + teacher_bias[0][None, None, None]
    )
    first_in = embed_tokens(noised, embed_in)
    alpha_end, sigma_end = plan(step_index - 2 * STRIDE)
    sigma_ratio = sigma_end / sigma_t
    packed = jnp.concatenate(
        [
            noised,
            step_index.astype(jnp.float32)[:, None],
            labels.astype(jnp.float32)[:, None],
            guide_level.astype(jnp.float32)[:, None],
        ],
        axis=1,
    )
    def student_normed(noised, steps, labels, guidance):
        rows = noised.shape[0] * seq_len
        label_rows = jnp.take(class_table, labels, axis=0).astype(jnp.float32)
        cond = sinusoid(steps, model_width) + label_rows + guidance[:, None] * guide_vec[None, :]
        modulation = cond[:, None, :] * student_gain[None] + student_bias[None]
        residual_in = embed_tokens(noised, embed_in).astype(jnp.float32)
        normed = (
            (layer_norm(residual_in) * (1.0 + modulation[:, 1, None, :]) + modulation[:, 0, None, :])
            .astype(jnp.bfloat16)
            .reshape(rows, model_width)
        )
        return residual_in, modulation[:, 2, None, :], normed

    def student_front(noised, steps, labels, guidance, student_up):
        residual_in, gate_rows, normed = student_normed(noised, steps, labels, guidance)
        pre_act = jnp.dot(normed, student_up, preferred_element_type=jnp.float32)
        hidden = jax.nn.gelu(pre_act, approximate=True).astype(jnp.bfloat16)
        return residual_in, gate_rows, normed, pre_act, hidden

    total = micro * dp_count
    element_count = total * width
    up_share = model_width // dp_count
    down_share = student_down.shape[0] // dp_count

    goal_scale = 1.0 / (alpha_end - sigma_ratio * alpha_t)
    up = lax.all_gather(teacher_up[0], "dp", axis=0, tiled=True)
    down = lax.all_gather(teacher_down[0], "dp", axis=0, tiled=True)
    ending = teacher_chain(
        first_in, noised, guidance, step_index, mods, up, down, embed_in, embed_out
    )
    goal_latent = (ending - sigma_ratio[:, None] * noised) * goal_scale[:, None]
    packed = lax.all_gather(packed, "dp", axis=0, tiled=True)
    own = student_front(noised, step_index, labels, guidance, student_up)
    partial_value = jnp.dot(own[4], student_down, preferred_element_type=jnp.float32)
    mixed = lax.psum(partial_value.astype(jnp.bfloat16), "section")
    all_mixed = lax.all_gather(mixed, "dp", axis=0, tiled=True)
    gathered = lax.all_gather(goal_latent, ("section", "dp"), axis=0, tiled=True)
    all_target = gathered[total * (section_count - 1):]
    all_mixed = all_mixed.reshape(total, seq_len, model_width)
    all_noised = packed[:, :width]
    all_steps = packed[:, width].astype(jnp.int32)
    all_labels = packed[:, width + 1].astype(jnp.int32)
    all_guidance = 0.5 * packed[:, width + 2]
    distill_target = lax.dynamic_slice_in_dim(all_target, dp_at * micro, micro, 0)

    def student_grads(operands, student_up, student_down):
        noised, steps, labels, guidance, mixed, target = operands
        count = noised.shape[0]
        rows = count * seq_len
        residual_in, gate_rows, normed, pre_act, hidden = student_front(
            noised, steps, labels, guidance, student_up
        )
        state_rows = residual_in + gate_rows * mixed.astype(jnp.float32)
        alpha_t, sigma_t = plan(steps)
        normed_out, pullback = jax.vjp(layer_norm, state_rows)
        predicted = jnp.dot(
            normed_out.astype(jnp.bfloat16).reshape(rows, model_width),
            embed_out,
            preferred_element_type=jnp.float32,
        ).reshape(count, width)
        estimate = alpha_t[:, None] * noised - sigma_t[:, None] * predicted
        weight = jnp.maximum(alpha_t * alpha_t / (sigma_t * sigma_t), 1.0)
        slope_pred = -2.0 / element_count * (sigma_t * weight)[:, None] * (estimate - target)
        back_norm = jnp.dot(
            slope_pred.reshape(rows, CH),
            embed_out.astype(jnp.float32).T,
            precision=lax.Precision.HIGHEST,
        )
        back_state = pullback(back_norm.reshape(count, seq_len, model_width))[0]
        back_part = (gate_rows * back_state).astype(jnp.bfloat16).reshape(rows, model_width)
        back_hidden = lax.dot_general(
            back_part, student_down, (((1,), (1,)), ((), ())), preferred_element_type=jnp.float32
        )
        back_pre = (back_hidden * gelu_slope(pre_act)).astype(jnp.bfloat16)
        normed_share = lax.dynamic_slice_in_dim(normed, dp_at * up_share, up_share, 1)
        hidden_share = lax.dynamic_slice_in_dim(hidden, dp_at * down_share, down_share, 1)
        contract_rows = (((0,), (0,)), ((), ()))
        return (
            lax.dot_general(
                normed_share, back_pre, contract_rows, preferred_element_type=jnp.float32
            ),
            lax.dot_general(
                hidden_share, back_part, contract_rows, preferred_element_type=jnp.float32
            ),
        )

    operands = [all_noised, all_steps, all_labels, all_guidance, all_mixed, all_target]
    grad_up, grad_down = run_chunks(
        max(1, dp_count // 8), student_grads, operands, (student_up, student_down)
    )
    return (distill_target, grad_up, grad_down)


def solution(mesh):
    return jax.shard_map(
        body,
        mesh=mesh,
        in_specs=(
            P("dp", None),
            P("dp", None),
            P("dp"),
            P("dp"),
            P("dp"),
            P(),
            P(),
            P(),
            P("section", "dp", None),
            P("section", "dp", None),
            P("section", None, None),
            P("section", None, None),
            P(None, "section"),
            P("section", None),
            P(),
            P(),
            P(),
        ),
        out_specs=(P("dp", None), P("dp", "section"), P(("section", "dp"), None)),
        check_vma=False,
    )
```

```python
import functools
import math

import jax
import jax.numpy as jnp
import numpy as np
from jax import lax
from jax.experimental import pallas as pl
from jax.experimental.pallas import tpu as pltpu
from jax.sharding import PartitionSpec as P

CH = 16
TSTEPS = 1000
STRIDE = 125


norm_eps = 1e-06


def shifted(shard, axis, by):
    length = lax.axis_size(axis)
    return lax.ppermute(shard, axis, [(i, (i + by) % length) for i in range(length)])


def from_root(shard, axis, root):
    mine = lax.axis_index(axis) == root
    return lax.psum(jnp.where(mine, shard, jnp.zeros_like(shard)), axis)


def layer_norm(values):
    center = values - jnp.mean(values, axis=-1, keepdims=True)
    spread = jnp.mean(center * center, axis=-1, keepdims=True)
    return center * lax.rsqrt(spread + norm_eps)


def sinusoid(step_ids, model_width):
    half_width = model_width // 2
    frequency = jnp.exp(-math.log(10000.0) * jnp.arange(half_width, dtype=jnp.float32) / half_width)
    phase_arg = step_ids.astype(jnp.float32)[:, None] * frequency[None, :]
    return jnp.concatenate([jnp.cos(phase_arg), jnp.sin(phase_arg)], axis=-1)


def plan(step_ids):
    angle_t = 0.5 * math.pi / TSTEPS * step_ids.astype(jnp.float32)
    return (jnp.cos(angle_t), jnp.sin(angle_t))


def embed_tokens(latent, embed_in):
    leading = latent.shape[0]
    patches = latent.reshape(leading * (latent.shape[1] // CH), CH).astype(jnp.bfloat16)
    tokens = jnp.dot(patches, embed_in, preferred_element_type=jnp.float32)
    return tokens.reshape(leading, latent.shape[1] // CH, embed_in.shape[1]).astype(jnp.bfloat16)


def mlp_block(inputs, modulation, up_proj, down_proj):
    groups, seq_len, model_width = inputs.shape
    residual_in = inputs.astype(jnp.float32)
    shift_rows = modulation[:, 0, None, :]
    scale_rows = modulation[:, 1, None, :]
    gate_rows = modulation[:, 2, None, :]
    normed = (layer_norm(residual_in) * (1.0 + scale_rows) + shift_rows).astype(jnp.bfloat16)
    pre_act = jnp.dot(
        normed.reshape(groups * seq_len, model_width), up_proj, preferred_element_type=jnp.float32
    )
    hidden = jax.nn.gelu(pre_act, approximate=True).astype(jnp.bfloat16)
    mixed = jnp.dot(hidden, down_proj, preferred_element_type=jnp.float32).reshape(
        groups, seq_len, model_width
    )
    return (residual_in + gate_rows * mixed).astype(jnp.bfloat16)


def velocity(states, embed_out):
    groups, seq_len, model_width = states.shape
    normed = layer_norm(states.astype(jnp.float32)).astype(jnp.bfloat16)
    result = jnp.dot(
        normed.reshape(groups * seq_len, model_width), embed_out, preferred_element_type=jnp.float32
    )
    return result.reshape(groups, seq_len * embed_out.shape[1])


def ddim_step(latent, predicted, time_now, time_next):
    alpha_now, sigma_now = plan(time_now)
    alpha_next, sigma_next = plan(time_next)
    clean_est = alpha_now[:, None] * latent - sigma_now[:, None] * predicted
    noise_est = sigma_now[:, None] * latent + alpha_now[:, None] * predicted
    return alpha_next[:, None] * clean_est + sigma_next[:, None] * noise_est


def gelu_slope(pre_act):
    return jax.vjp(lambda inner: jax.nn.gelu(inner, approximate=True), pre_act)[1](
        jnp.ones_like(pre_act)
    )[0]


def run_chunks(count, one, operands, shared):
    if count == 1:
        return one(operands, *shared)

    def step(carry, piece):
        out = one(piece, *shared)
        return (carry[0] + out[0], carry[1] + out[1]), None

    split = [a.reshape((count, a.shape[0] // count) + a.shape[1:]) for a in operands]
    shapes = jax.eval_shape(one, [a[0] for a in split], *shared)
    zeros = tuple(jnp.zeros(s.shape, s.dtype) for s in shapes)
    return lax.scan(step, zeros, split)[0]


def teacher_chain(first_in, noised, guidance, step_index, mods, up, down, embed_in, embed_out):
    section_count = lax.axis_size("section")
    section_at = lax.axis_index("section")
    micro, seq_len, model_width = first_in.shape

    def paired(tokens):
        return jnp.broadcast_to(tokens[:, None], (micro, 2, seq_len, model_width)).reshape(
            2 * micro, seq_len, model_width
        )

    latent = noised
    states = paired(first_in)
    for which_step in range(2):
        mod = mods[which_step].reshape(2 * micro, 3, model_width)
        if which_step:
            states = paired(embed_tokens(latent, embed_in))
        for layer in range(section_count):
            states = mlp_block(states, mod, up, down)
            if layer < section_count - 1:
                states = lax.ppermute(states, "section", [(layer, layer + 1)])
        predicted = velocity(states, embed_out).reshape(micro, 2, -1)
        weight = guidance[:, None]
        guided = (1.0 + weight) * predicted[:, 0] - weight * predicted[:, 1]
        time_now = step_index - which_step * STRIDE
        stepped = ddim_step(latent, guided, time_now, time_now - STRIDE)
        if which_step == 0:
            returned = lax.ppermute(
                stepped, "section", [(section_count - 1, 0)]
            )
            latent = jnp.where(section_at == section_count - 1, stepped, returned)
    return stepped


def cos_of(angle, shift_quarter):
    quarters = jnp.floor(angle * (2.0 / math.pi) + 0.5)
    rest = ((angle - quarters * 1.5703125) - quarters * 4.837512969970703125e-4) - (
        quarters * 7.549789954891882e-8
    )
    turn = quarters - shift_quarter
    turn = turn - 4.0 * jnp.floor(turn * 0.25)
    square = rest * rest
    sine = rest + rest * square * (
        -1.6666654611e-1 + square * (8.3321608736e-3 - 1.9515295891e-4 * square)
    )
    cosine = (
        1.0
        - 0.5 * square
        + square
        * square
        * (4.166664568298827e-2 + square * (-1.388731625493765e-3 + 2.443315711809948e-5 * square))
    )
    odd = (turn == 1.0) | (turn == 3.0)
    negative = (turn == 1.0) | (turn == 2.0)
    value = jnp.where(odd, sine, cosine)
    return jnp.where(negative, -value, value)


NT = (((1,), (1,)), ((), ()))
GELU_A = math.sqrt(2.0 / math.pi)
GELU_B = 0.044715


def dot32(a, b, dims=(((1,), (0,)), ((), ()))):
    return lax.dot_general(a, b, dims, preferred_element_type=jnp.float32)


def gelu_pair(pre):
    square = pre * pre
    bent = jnp.tanh(GELU_A * (pre + GELU_B * square * pre))
    half = 0.5 * (1.0 + bent)
    slope = half + 0.5 * pre * (1.0 - bent * bent) * (GELU_A * (1.0 + 3.0 * GELU_B * square))
    return pre * half, slope


def token_mask(first, count, shape):
    lane = lax.broadcasted_iota(jnp.int32, shape, 1) // CH
    return [lane == first + k for k in range(count)]


def spread(values, first, count):
    masks = token_mask(first, count, values.shape)
    zero = jnp.zeros_like(values)
    return jnp.concatenate([jnp.where(m, values, zero) for m in masks], axis=0)


def gathered_tokens(values, first, count, rows):
    masks = token_mask(first, count, (rows, values.shape[1]))
    total = jnp.zeros((rows, values.shape[1]), jnp.float32)
    for k in range(count):
        total = total + jnp.where(masks[k], values[k * rows : (k + 1) * rows], 0.0)
    return total


def mega_kernel(
    dims,
    steps_in, labels_in, levels_in, clean_in, noise_in, up_shard, down_shard, t_gain, t_bias, s_gain, s_bias, guide_vec, freq,
    embed_in, embed_out_t, stud_up_hbm, stud_down_hbm, table_hbm,
    target_out, grad_up, grad_down,
    stud_up, stud_down, table, packed, up, down, tiled_in, tiled_out,
    noised, cols, wave, labs, scond, tok, slope, n_share, h_share, parts, pair_in, pair_sum,
    cross_in, mixed, xhat, rstd, pred, states, outs, latents, velo, target_all, hid,
    local_sem, send, recv, move_send, move_recv, z_send, z_recv, t_send, t_recv, gate,
):
    sections, dps, micro, seq_len = dims
    total = dps * micro
    width = clean_in.shape[1]
    model = embed_in.shape[1]
    sec = lax.axis_index("section")
    me = lax.axis_index("dp")
    z, y = me // 2, me % 2
    core, side = sec % 2, z // 2
    tail = sections - 1
    mid_z, end_z, far_mid_z = 1 + side, 3 * side, 2 - side
    far_end_z = 3 - end_z
    is_mid = z == mid_z
    is_end = z == end_z
    oy = 1 - y
    E_y, E_o = end_z * 2 + y, end_z * 2 + oy
    A_y, A_o = mid_z * 2 + y, mid_z * 2 + oy
    B_y, B_o = far_mid_z * 2 + y, far_mid_z * 2 + oy
    F_y, F_o = far_end_z * 2 + y, far_end_z * 2 + oy
    MESH = pl.DeviceIdType.MESH
    devices = sections * dps
    mine = sec * dps + me

    barrier = pltpu.get_barrier_semaphore()

    def greet(k, carry):
        other = lax.rem(mine + k, devices)
        pl.semaphore_signal(
            barrier, inc=1, device_id={"section": other // dps, "dp": lax.rem(other, dps)},
            device_id_type=MESH,
        )
        return carry

    def place(who):
        zz, yy = who // 2, who % 2
        return (zz % 2) * (dps // 2) + (zz // 2) * 2 + yy

    lax.fori_loop(1, devices, greet, 0)
    row = lax.broadcasted_iota(jnp.int32, (micro, 128), 0)
    column = lax.broadcasted_iota(jnp.int32, (micro, 128), 1)
    cells = jnp.zeros((micro, 128), jnp.float32)
    for k, ref in enumerate((steps_in, labels_in, levels_in)):
        for b in range(micro):
            cells = jnp.where((row == b) & (column == k), ref[b].astype(jnp.float32), cells)
    slot = place(me)
    packed[slot, :, 0:width] = clean_in[...]
    packed[slot, :, width : 2 * width] = noise_in[...]
    packed[slot, :, 2 * width :] = cells
    locals_ = [
        pltpu.make_async_copy(stud_up_hbm, stud_up, local_sem.at[0]),
        pltpu.make_async_copy(stud_down_hbm, stud_down, local_sem.at[1]),
        pltpu.make_async_copy(table_hbm, table, local_sem.at[2]),
    ]
    ur, dr = up_shard.shape[0], down_shard.shape[0]

    def urow(who):
        return up.at[pl.ds(pl.multiple_of(who * ur, 16), ur)]

    def drow(who, lo=0, n=None):
        return down.at[pl.ds(pl.multiple_of(who * dr + lo, 16), dr if n is None else n)]

    shards = [
        pltpu.make_async_copy(up_shard, urow(me), local_sem.at[3]),
        pltpu.make_async_copy(down_shard, drow(me), local_sem.at[4]),
    ]
    for c in shards + locals_:
        c.start()
    pl.semaphore_wait(barrier, devices - 1)

    def copy(i, src, dst, **device):
        return pltpu.make_async_remote_copy(
            src_ref=src, dst_ref=dst, send_sem=send.at[i], recv_sem=recv.at[i],
            device_id=device, device_id_type=MESH,
        )

    packs = [
        copy(k - 1, packed.at[slot], packed.at[slot], dp=lax.rem(me + k, dps))
        for k in range(1, dps)
    ]
    for c in packs:
        c.start()
    base = dps - 1
    names = [
        "ey_u", "ey_d", "ez_u", "ez_d", "ezo_u", "ezo_d", "ezo_r", "det1", "det2", "det3",
        "ay_u", "ay_d", "am_u", "am_d", "ame_u", "ame_d", "amo",
        "ayf_u", "ayf_d", "aye_u", "aye_d", "pair", "cross", "back",
    ]
    index = {n: base + k for k, n in enumerate(names)}
    cut = (2 * dr // 3) // 16 * 16
    low, high = (0, cut), (cut, dr - cut)
    span = {"ezo_d": low, "ezo_r": high, "det1": low, "det2": low, "det3": low, "amo": low, "ay_d": high, "aye_d": high}

    def piece(name, who, dst):
        ref = urow(who) if name.endswith("u") else drow(who, *span.get(name, (0, dr)))
        return copy(index[name], ref, ref, dp=dst)

    end_sends = (("ez_u", A_y), ("ey_u", E_o), ("ez_d", A_y), ("ey_d", E_o))
    mid_sends = (
        ("am_u", B_y), ("ay_u", A_o), ("det1", E_y), ("am_d", B_y), ("ay_d", A_o)
    )

    def begin():
        @pl.when(is_end)
        def _():
            for n, dst in end_sends:
                piece(n, me, dst).start()

        @pl.when(is_mid)
        def _():
            for n, dst in mid_sends:
                piece(n, me, dst).start()

    def relay(part):
        @pl.when(is_end)
        def _():
            piece("ey_" + part, E_o, E_o).wait_recv()
            piece("ezo_" + part, E_o, A_y).start()
            if part == "d":
                piece("ezo_r", E_o, A_y).start()
            if part == "u":
                piece("det1", A_y, E_o).wait_recv()
                piece("det2", A_y, E_o).start()
            else:
                piece("det2", A_o, A_y).wait_recv()
                piece("det3", A_o, A_y).start()

        @pl.when(is_mid)
        def _():
            piece("ez_" + part, E_y, B_y).wait_recv()
            piece("ame_" + part, E_y, B_y).start()
            piece("am_" + part, B_y, A_o).wait_recv()
            piece("ayf_" + part, B_y, A_o).start()

    def third():
        @pl.when(is_mid)
        def _():
            piece("ame_u", F_y, A_o).wait_recv()
            piece("aye_u", F_y, A_o).start()

    def fourth():
        @pl.when(is_mid)
        def _():
            piece("ezo_d", E_o, B_y).wait_recv()
            piece("amo", E_o, B_y).start()
            piece("ame_d", F_y, A_o).wait_recv()
            piece("aye_d", F_y, A_o).start()

    sibling = sec + 1 - 2 * core

    for c in shards:
        c.wait()

    @pl.when(core == 0)
    def _():
        begin()

    for k in range(seq_len):
        tiled_in[k * CH : (k + 1) * CH] = embed_in[...]
        tiled_out[k * CH : (k + 1) * CH] = embed_out_t[...]
    lane_model = lax.broadcasted_iota(jnp.int32, (1, model), 1)
    sine_lane = jnp.where(lane_model >= model // 2, 1.0, 0.0)
    for c in packs:
        c.wait_recv()
    data = packed[...].reshape(total, packed.shape[2])
    steps = data[:, 2 * width : 2 * width + 1]
    label = data[:, 2 * width + 1 : 2 * width + 2]
    guide = 0.5 * data[:, 2 * width + 2 : 2 * width + 3]
    for k in range(3):
        angle = jnp.broadcast_to(
            (0.5 * math.pi / TSTEPS) * (steps - float(k * STRIDE)), (total, 128)
        )
        cols[2 * k] = cos_of(angle, 0.0)
        cols[2 * k + 1] = cos_of(angle, 1.0)
    cols[6] = jnp.broadcast_to(guide, (total, 128))
    alpha_t, sigma_t = cols[0][:, 0:1], cols[1][:, 0:1]
    clean = alpha_t * data[:, :width] + sigma_t * data[:, width : 2 * width]
    noised[...] = clean
    for k in range(2):
        wave[k] = cos_of((steps - float(k * STRIDE)) * freq[...], sine_lane)
    for c in locals_:
        c.wait()
    classes = table.shape[0] - 1
    whole = (classes // 16) * 16
    ids = lax.broadcasted_iota(jnp.int32, (total, whole), 1).astype(jnp.float32)
    rows = dot32(jnp.where(ids == label, 1.0, 0.0).astype(jnp.bfloat16), table[:whole])
    rest = table[whole:].astype(jnp.float32)
    for k in range(classes - whole):
        rows = rows + jnp.where(label == float(whole + k), rest[k : k + 1], 0.0)
    labs[0] = rows
    labs[1] = jnp.broadcast_to(rest[classes - whole : classes - whole + 1], (total, model))
    vector = jnp.concatenate([guide_vec[k : k + 1] for k in range(model // 128)], axis=1)
    scond[...] = wave[0] + rows + guide * vector

    block = seq_len // 2
    blocks = 4
    group = total // 2
    brows = block * group
    share = n_share.shape[0]
    pick = jnp.where(
        lax.broadcasted_iota(jnp.int32, (share, model), 1)
        == lax.broadcasted_iota(jnp.int32, (share, model), 0) + me * share,
        1.0, 0.0,
    ).astype(jnp.bfloat16)

    def at_block(i):
        return pl.ds(pl.multiple_of(i * brows, brows), brows)

    def members(i):
        return pl.ds(pl.multiple_of((i // 2) * group, group), group)

    def first_of(i):
        return lax.rem(i, 2) * block

    def student_part(i, k):
        return scond[members(i)] * s_gain[k : k + 1] + s_bias[k : k + 1]

    def front(i, carry):
        here = at_block(i)
        tokens = dot32(
            spread(noised[members(i)], first_of(i), block).astype(jnp.bfloat16), tiled_in[...]
        ).astype(jnp.bfloat16)
        tok[here] = tokens
        cube = layer_norm(tokens.astype(jnp.float32)).reshape(block, group, model)
        normed = (cube * (1.0 + student_part(i, 1))[None] + student_part(i, 0)[None]).astype(
            jnp.bfloat16
        )
        normed = normed.reshape(brows, model)
        n_share[:, here] = dot32(pick, normed, NT).astype(jnp.bfloat16)
        hidden, bend = gelu_pair(dot32(normed, stud_up[...]))
        hidden = hidden.astype(jnp.bfloat16)
        slope[here] = bend
        h_share[:, here] = dot32(pick, hidden, NT).astype(jnp.bfloat16)
        parts[here] = dot32(hidden, stud_down[...]).astype(jnp.bfloat16)
        return carry

    lax.fori_loop(0, blocks // 2, front, 0)

    @pl.when(core == 0)
    def _():
        relay("u")

    lax.fori_loop(blocks // 2, blocks, front, 0)

    half_rows = seq_len * total // 2

    def half_of(ref, c):
        return ref.at[pl.ds(pl.multiple_of(c * half_rows, half_rows), half_rows)]

    pair = copy(index["pair"], half_of(parts, 1 - core), pair_in, section=sibling)
    cross = copy(index["cross"], pair_sum, cross_in, section=lax.rem(sec + 2, sections))
    back = copy(index["back"], half_of(mixed, core), half_of(mixed, core), section=sibling)
    pair.start()

    @pl.when(core == 0)
    def _():
        relay("d")
        pl.semaphore_signal(
            gate, inc=1, device_id={"section": sibling}, device_id_type=MESH
        )

    pair.wait_recv()
    pair_sum[...] = (
        half_of(parts, core)[...].astype(jnp.float32) + pair_in[...].astype(jnp.float32)
    ).astype(jnp.bfloat16)
    cross.start()

    @pl.when(core == 0)
    def _():
        third()

    turned = model // 4

    def turn(i, carry):
        here = pl.ds(pl.multiple_of(i * turned, turned), turned)
        eye = jnp.where(
            lax.broadcasted_iota(jnp.int32, (turned, model), 1)
            == lax.broadcasted_iota(jnp.int32, (turned, model), 0) + i * turned,
            1.0, 0.0,
        ).astype(jnp.bfloat16)
        stud_up[here] = dot32(eye, stud_down[...], NT).astype(jnp.bfloat16)
        return carry

    lax.fori_loop(0, 4, turn, 0)

    @pl.when(core == 0)
    def _():
        fourth()

    @pl.when(core == 1)
    def _():
        pl.semaphore_wait(gate, 1)
        begin()
        relay("u")

    cross.wait_recv()
    mixed[pl.ds(pl.multiple_of(core * half_rows, half_rows), half_rows)] = (
        pair_sum[...].astype(jnp.float32) + cross_in[...].astype(jnp.float32)
    ).astype(jnp.bfloat16)
    back.start()

    @pl.when(core == 1)
    def _():
        relay("d")

    back.wait_recv()
    pred[...] = jnp.zeros_like(pred)

    def middle(i, carry):
        here = at_block(i)
        state = tok[here].astype(jnp.float32).reshape(block, group, model) + student_part(i, 2)[
            None
        ] * mixed[here].astype(jnp.float32).reshape(block, group, model)
        state = state.reshape(brows, model)
        center = state - jnp.mean(state, axis=-1, keepdims=True)
        inverse = lax.rsqrt(jnp.mean(center * center, axis=-1, keepdims=True) + norm_eps)
        unit = center * inverse
        xhat[here] = unit
        rstd[here] = jnp.broadcast_to(inverse, (brows, 128))
        pred[members(i)] += gathered_tokens(
            dot32(unit.astype(jnp.bfloat16), tiled_out[...], NT), first_of(i), block, group
        )
        return carry

    lax.fori_loop(0, blocks // 2, middle, 0)

    @pl.when(core == 1)
    def _():
        third()

    lax.fori_loop(blocks // 2, blocks, middle, 0)

    @pl.when(core == 1)
    def _():
        fourth()

    trows = micro * seq_len
    chunk = 768 if up.shape[1] % 768 == 0 else up.shape[1]

    def owned(j):
        return j * (dps // 2) + (z - 1) * 2 + y

    def sample_rows(d):
        return pl.ds(pl.multiple_of(d * micro, micro), micro)

    def move(i):
        return pltpu.make_async_remote_copy(
            src_ref=outs.at[i], dst_ref=states.at[i],
            send_sem=move_send.at[i], recv_sem=move_recv.at[i],
            device_id={"section": lax.rem(sec + 1, sections)}, device_id_type=MESH,
        )

    def back_move(j):
        return pltpu.make_async_remote_copy(
            src_ref=latents.at[1, j], dst_ref=latents.at[1, j],
            send_sem=z_send.at[j], recv_sem=z_recv.at[j],
            device_id={"section": 0}, device_id_type=MESH,
        )

    def target_copy(k, j, d):
        other = lax.rem(mine + k, devices)
        return pltpu.make_async_remote_copy(
            src_ref=target_all.at[d], dst_ref=target_all.at[d],
            send_sem=t_send.at[j * devices + k], recv_sem=t_recv.at[d],
            device_id={"section": other // dps, "dp": lax.rem(other, dps)}, device_id_type=MESH,
        )

    @pl.when(is_mid)
    def _():
        for n, who in (("ay_u", A_o), ("ayf_u", B_o), ("ezo_u", E_o), ("aye_u", F_o)):
            piece(n, who, A_o).wait_recv()
        for j in range(2):
            latents[0, j] = noised[sample_rows(owned(j))]

        def task(i, carry):
            step, j, half = i // 4, lax.rem(i // 2, 2), lax.rem(i, 2)
            d = owned(j)
            here = sample_rows(d)

            @pl.when(sec == 0)
            def _():
                @pl.when((step == 1) & (half == 0))
                def _():
                    back_move(j).wait_recv()

                states[i] = dot32(
                    spread(latents[step, j], 0, seq_len).astype(jnp.bfloat16), tiled_in[...]
                ).astype(jnp.bfloat16)

            @pl.when(sec > 0)
            def _():
                move(i).wait_recv()

            cond = wave[step, here] + labs[half, here]
            residual = states[i].astype(jnp.float32)
            cube = layer_norm(residual).reshape(seq_len, micro, model)
            scale = cond * t_gain[1] + t_bias[1]
            shift = cond * t_gain[0] + t_bias[0]
            gate = cond * t_gain[2] + t_bias[2]
            normed = (cube * (1.0 + scale)[None] + shift[None]).astype(jnp.bfloat16)
            normed = normed.reshape(trows, model)
            for k in range(up.shape[1] // chunk):
                hid[:, k * chunk : (k + 1) * chunk] = jax.nn.gelu(
                    dot32(normed, up[:, k * chunk : (k + 1) * chunk]), approximate=True
                ).astype(jnp.bfloat16)

            @pl.when(i == 0)
            def _():
                for n, who in (
                    ("ay_d", A_o), ("det3", A_o), ("ayf_d", B_o), ("aye_d", F_o), ("amo", F_o),
                    ("ezo_r", E_o),
                ):
                    piece(n, who, A_o).wait_recv()

            acc = dot32(hid[...], down[...])
            out = residual.reshape(seq_len, micro, model) + gate[None] * acc.reshape(
                seq_len, micro, model
            )
            outs[i] = out.reshape(trows, model).astype(jnp.bfloat16)

            @pl.when(sec < tail)
            def _():
                move(i).start()

            @pl.when(sec == tail)
            def _():
                last = layer_norm(outs[i].astype(jnp.float32)).astype(jnp.bfloat16)
                velo[half] = gathered_tokens(
                    dot32(last, tiled_out[...], NT), 0, seq_len, micro
                )

                @pl.when(half == 1)
                def _():
                    level = cols[6, here][:, 0:1]
                    guided = (1.0 + level) * velo[0] - level * velo[1]
                    a_now = cols[2 * step, here][:, 0:1]
                    s_now = cols[2 * step + 1, here][:, 0:1]
                    a_next = cols[2 * step + 2, here][:, 0:1]
                    s_next = cols[2 * step + 3, here][:, 0:1]
                    before = latents[step, j]
                    after = a_next * (a_now * before - s_now * guided) + s_next * (
                        s_now * before + a_now * guided
                    )

                    @pl.when(step == 0)
                    def _():
                        latents[1, j] = after
                        back_move(j).start()

                    @pl.when(step == 1)
                    def _():
                        a_first, s_first = cols[0, here][:, 0:1], cols[1, here][:, 0:1]
                        ratio = s_next / s_first
                        target_all[d] = (after - ratio * latents[0, j]) / (a_next - ratio * a_first)

                        def tell(k, carry):
                            target_copy(k, j, d).start()
                            return carry

                        lax.fori_loop(1, devices, tell, 0)

            return carry

        lax.fori_loop(0, 8, task, 0)

    grad_up[...] = jnp.zeros_like(grad_up)
    grad_down[...] = jnp.zeros_like(grad_down)

    def finish(i, carry):
        here = at_block(i)
        slopes = dot32(
            spread(pred[members(i)], first_of(i), block).astype(jnp.bfloat16), tiled_out[...]
        ) + dot32(
            spread(noised[members(i)], first_of(i), block).astype(jnp.bfloat16), tiled_out[...]
        )
        unit = xhat[here]
        mean = jnp.mean(slopes, axis=-1, keepdims=True)
        along = jnp.mean(slopes * unit, axis=-1, keepdims=True)
        back_state = rstd[here][:, 0:1] * (slopes - mean - unit * along)
        back_part = (student_part(i, 2)[None] * back_state.reshape(block, group, model)).astype(
            jnp.bfloat16
        ).reshape(brows, model)
        grad_down[...] += dot32(h_share[:, here], back_part)
        back_pre = (dot32(back_part, stud_up[...]) * slope[here]).astype(jnp.bfloat16)
        grad_up[...] += dot32(n_share[:, here], back_pre)
        return carry

    for part in range(2):
        for k in range(dps // 2):
            d = part * (dps // 2) + k

            @pl.when(jnp.logical_not((sec == tail) & (z == 1 + k // 2) & (y == k % 2)))
            def _():
                target_copy(1, 0, d).wait_recv()

        these = pl.ds(part * group, group)
        alpha_h, sigma_h = cols[0, these][:, 0:1], cols[1, these][:, 0:1]
        weight = jnp.maximum(alpha_h * alpha_h / (sigma_h * sigma_h), 1.0)
        estimate = alpha_h * noised[these] - sigma_h * pred[these]
        goal = target_all[pl.ds(part * (dps // 2), dps // 2)].reshape(group, width)
        seed = (-2.0 / (total * width)) * (sigma_h * weight) * (estimate - goal)
        seed_hi = seed.astype(jnp.bfloat16).astype(jnp.float32)
        pred[these] = seed_hi
        noised[these] = seed - seed_hi
        lax.fori_loop(2 * part, 2 * part + 2, finish, 0)

    target_out[...] = target_all[slot]

    for c in packs + [pair, cross, back]:
        c.wait_send()

    @pl.when(is_end)
    def _():
        for n, dst in end_sends:
            piece(n, me, dst).wait_send()
        for n, who, dst in (
            ("ezo_u", E_o, A_y), ("ezo_d", E_o, A_y), ("ezo_r", E_o, A_y),
            ("det2", A_y, E_o), ("det3", A_o, A_y),
        ):
            piece(n, who, dst).wait_send()

    @pl.when(is_mid)
    def _():
        for n, dst in mid_sends:
            piece(n, me, dst).wait_send()
        for n, who, dst in (
            ("ame_u", E_y, B_y), ("ame_d", E_y, B_y), ("amo", E_o, B_y),
            ("ayf_u", B_y, A_o), ("ayf_d", B_y, A_o), ("aye_u", F_y, A_o), ("aye_d", F_y, A_o),
        ):
            piece(n, who, dst).wait_send()

        @pl.when(sec < tail)
        def _():
            def done(i, carry):
                move(i).wait_send()
                return carry

            lax.fori_loop(0, 8, done, 0)

        @pl.when(sec == tail)
        def _():
            for j in range(2):
                back_move(j).wait_send()

                def told(k, carry):
                    target_copy(k, j, owned(j)).wait_send()
                    return carry

                lax.fori_loop(1, devices, told, 0)


def flush_kernel(a, b, c, x, y, z):
    x[...] = a[...]
    y[...] = b[...]
    z[...] = c[...]


def mega_call(dims, operands):
    sections, dps, micro, seq_len = dims
    clean, up_shard, down_shard = operands[3], operands[5], operands[6]
    hidden, model = up_shard.shape[1], down_shard.shape[1]
    stud_up, stud_down, table = operands[-3:]
    width = clean.shape[1]
    total = dps * micro
    rows = total * seq_len
    trows = micro * seq_len
    share_up, share_down = model // dps, stud_down.shape[0] // dps
    f32, bf16 = jnp.float32, jnp.bfloat16
    vmem = pl.BlockSpec(memory_space=pltpu.VMEM)
    hbm = pl.BlockSpec(memory_space=pl.ANY)
    smem = pl.BlockSpec(memory_space=pltpu.SMEM)
    V, D = pltpu.VMEM, pltpu.SemaphoreType.DMA
    results = pl.pallas_call(
        functools.partial(mega_kernel, dims),
        out_shape=(
            jax.ShapeDtypeStruct((micro, width), f32),
            jax.ShapeDtypeStruct((share_up, stud_up.shape[1]), f32),
            jax.ShapeDtypeStruct((share_down, model), f32),
        ),
        in_specs=[smem] * 3 + [vmem] * 2 + [hbm] * 2 + [vmem] * (len(operands) - 10) + [hbm] * 3,
        out_specs=(vmem,) * 3,
        scratch_shapes=[
            V(stud_up.shape, bf16), V(stud_down.shape, bf16), V(table.shape, bf16),
            V((dps, micro, 2 * width + 128), f32),
            V((up_shard.shape[0] * dps, hidden), bf16),
            V((down_shard.shape[0] * dps, model), bf16),
            V((width, model), bf16), V((width, model), bf16),
            V((total, width), f32), V((7, total, 128), f32),
            V((2, total, model), f32), V((2, total, model), f32), V((total, model), f32),
            V((rows, model), bf16), V((rows, model), f32),
            V((share_up, rows), bf16), V((share_down, rows), bf16),
            V((rows, model), bf16), V((rows // 2, model), bf16), V((rows // 2, model), bf16),
            V((rows // 2, model), bf16), V((rows, model), bf16),
            V((rows, model), f32), V((rows, 128), f32), V((total, width), f32),
            V((8, trows, model), bf16), V((8, trows, model), bf16),
            V((2, 2, micro, width), f32), V((2, micro, width), f32), V((dps, micro, width), f32),
            V((trows, hidden), bf16),
            D((5,)), D((32,)), D((32,)), D((8,)), D((8,)), D((2,)), D((2,)),
            D((2 * sections * dps,)), D((dps,)), pltpu.SemaphoreType.REGULAR,
        ],
        compiler_params=pltpu.CompilerParams(
            collective_id=0, has_side_effects=True, vmem_limit_bytes=63 << 20
        ),
    )(*operands)
    return pl.pallas_call(
        flush_kernel,
        out_shape=tuple(jax.ShapeDtypeStruct(r.shape, r.dtype) for r in results),
        in_specs=[vmem] * 3,
        out_specs=(vmem,) * 3,
    )(*results)


def body(
    clean_latent,
    noise_draw,
    step_index,
    labels,
    guide_level,
    class_table,
    embed_in,
    embed_out,
    teacher_up,
    teacher_down,
    teacher_gain,
    teacher_bias,
    student_up,
    student_down,
    student_gain,
    student_bias,
    guide_vec,
):
    section_count = lax.axis_size("section")
    dp_count = lax.axis_size("dp")
    section_at = lax.axis_index("section")
    dp_at = lax.axis_index("dp")
    micro = clean_latent.shape[0]
    width = clean_latent.shape[1]
    seq_len = width // CH
    model_width = class_table.shape[1]
    fused = (
        dp_count == 8
        and section_count == 4
        and micro == 8
        and seq_len % 4 == 0
        and width % 128 == 0
        and model_width % 128 == 0
        and teacher_up.shape[1] % 16 == 0
        and teacher_down.shape[1] % 16 == 0
        and student_up.shape[1] == student_down.shape[0] == model_width
    )
    if fused:
        half_width = model_width // 2
        frequency = np.exp(-math.log(10000.0) * np.arange(half_width) / half_width)
        frequency = np.tile(frequency, 2)[None].astype(np.float32)
        return mega_call(
            (section_count, dp_count, micro, seq_len),
            (
                step_index, labels, guide_level, clean_latent, noise_draw,
                teacher_up[0], teacher_down[0],
                teacher_gain.reshape(3, 1, model_width), teacher_bias.reshape(3, 1, model_width),
                student_gain, student_bias, guide_vec.reshape(model_width // 128, 128), jnp.asarray(frequency),
                embed_in, embed_out.T, student_up, student_down, class_table,
            ),
        )
    alpha_t, sigma_t = plan(step_index)
    noised = alpha_t[:, None] * clean_latent + sigma_t[:, None] * noise_draw
    guidance = 0.5 * guide_level.astype(jnp.float32)
    label_rows = jnp.take(class_table, labels, axis=0).astype(jnp.float32)
    null_row = class_table[class_table.shape[0] - 1].astype(jnp.float32)
    wave_rows = jnp.stack(
        [sinusoid(step_index - step_k * STRIDE, model_width) for step_k in range(2)]
    )
    conditions = jnp.stack(
        [wave_rows + label_rows[None], wave_rows + null_row[None, None, :]], axis=2
    )
    mods = (
        conditions[:, :, :, None, :] * teacher_gain[0][None, None, None]
        + teacher_bias[0][None, None, None]
    )
    first_in = embed_tokens(noised, embed_in)
    alpha_end, sigma_end = plan(step_index - 2 * STRIDE)
    sigma_ratio = sigma_end / sigma_t
    packed = jnp.concatenate(
        [
            noised,
            step_index.astype(jnp.float32)[:, None],
            labels.astype(jnp.float32)[:, None],
            guide_level.astype(jnp.float32)[:, None],
        ],
        axis=1,
    )
    def student_normed(noised, steps, labels, guidance):
        rows = noised.shape[0] * seq_len
        label_rows = jnp.take(class_table, labels, axis=0).astype(jnp.float32)
        cond = sinusoid(steps, model_width) + label_rows + guidance[:, None] * guide_vec[None, :]
        modulation = cond[:, None, :] * student_gain[None] + student_bias[None]
        residual_in = embed_tokens(noised, embed_in).astype(jnp.float32)
        normed = (
            (layer_norm(residual_in) * (1.0 + modulation[:, 1, None, :]) + modulation[:, 0, None, :])
            .astype(jnp.bfloat16)
            .reshape(rows, model_width)
        )
        return residual_in, modulation[:, 2, None, :], normed

    def student_front(noised, steps, labels, guidance, student_up):
        residual_in, gate_rows, normed = student_normed(noised, steps, labels, guidance)
        pre_act = jnp.dot(normed, student_up, preferred_element_type=jnp.float32)
        hidden = jax.nn.gelu(pre_act, approximate=True).astype(jnp.bfloat16)
        return residual_in, gate_rows, normed, pre_act, hidden

    total = micro * dp_count
    element_count = total * width
    up_share = model_width // dp_count
    down_share = student_down.shape[0] // dp_count

    goal_scale = 1.0 / (alpha_end - sigma_ratio * alpha_t)
    up = lax.all_gather(teacher_up[0], "dp", axis=0, tiled=True)
    down = lax.all_gather(teacher_down[0], "dp", axis=0, tiled=True)
    ending = teacher_chain(
        first_in, noised, guidance, step_index, mods, up, down, embed_in, embed_out
    )
    goal_latent = (ending - sigma_ratio[:, None] * noised) * goal_scale[:, None]
    packed = lax.all_gather(packed, "dp", axis=0, tiled=True)
    own = student_front(noised, step_index, labels, guidance, student_up)
    partial_value = jnp.dot(own[4], student_down, preferred_element_type=jnp.float32)
    mixed = lax.psum(partial_value.astype(jnp.bfloat16), "section")
    all_mixed = lax.all_gather(mixed, "dp", axis=0, tiled=True)
    gathered = lax.all_gather(goal_latent, ("section", "dp"), axis=0, tiled=True)
    all_target = gathered[total * (section_count - 1):]
    all_mixed = all_mixed.reshape(total, seq_len, model_width)
    all_noised = packed[:, :width]
    all_steps = packed[:, width].astype(jnp.int32)
    all_labels = packed[:, width + 1].astype(jnp.int32)
    all_guidance = 0.5 * packed[:, width + 2]
    distill_target = lax.dynamic_slice_in_dim(all_target, dp_at * micro, micro, 0)

    def student_grads(operands, student_up, student_down):
        noised, steps, labels, guidance, mixed, target = operands
        count = noised.shape[0]
        rows = count * seq_len
        residual_in, gate_rows, normed, pre_act, hidden = student_front(
            noised, steps, labels, guidance, student_up
        )
        state_rows = residual_in + gate_rows * mixed.astype(jnp.float32)
        alpha_t, sigma_t = plan(steps)
        normed_out, pullback = jax.vjp(layer_norm, state_rows)
        predicted = jnp.dot(
            normed_out.astype(jnp.bfloat16).reshape(rows, model_width),
            embed_out,
            preferred_element_type=jnp.float32,
        ).reshape(count, width)
        estimate = alpha_t[:, None] * noised - sigma_t[:, None] * predicted
        weight = jnp.maximum(alpha_t * alpha_t / (sigma_t * sigma_t), 1.0)
        slope_pred = -2.0 / element_count * (sigma_t * weight)[:, None] * (estimate - target)
        back_norm = jnp.dot(
            slope_pred.reshape(rows, CH),
            embed_out.astype(jnp.float32).T,
            precision=lax.Precision.HIGHEST,
        )
        back_state = pullback(back_norm.reshape(count, seq_len, model_width))[0]
        back_part = (gate_rows * back_state).astype(jnp.bfloat16).reshape(rows, model_width)
        back_hidden = lax.dot_general(
            back_part, student_down, (((1,), (1,)), ((), ())), preferred_element_type=jnp.float32
        )
        back_pre = (back_hidden * gelu_slope(pre_act)).astype(jnp.bfloat16)
        normed_share = lax.dynamic_slice_in_dim(normed, dp_at * up_share, up_share, 1)
        hidden_share = lax.dynamic_slice_in_dim(hidden, dp_at * down_share, down_share, 1)
        contract_rows = (((0,), (0,)), ((), ()))
        return (
            lax.dot_general(
                normed_share, back_pre, contract_rows, preferred_element_type=jnp.float32
            ),
            lax.dot_general(
                hidden_share, back_part, contract_rows, preferred_element_type=jnp.float32
            ),
        )

    operands = [all_noised, all_steps, all_labels, all_guidance, all_mixed, all_target]
    grad_up, grad_down = run_chunks(
        max(1, dp_count // 8), student_grads, operands, (student_up, student_down)
    )
    return (distill_target, grad_up, grad_down)


def solution(mesh):
    return jax.shard_map(
        body,
        mesh=mesh,
        in_specs=(
            P("dp", None),
            P("dp", None),
            P("dp"),
            P("dp"),
            P("dp"),
            P(),
            P(),
            P(),
            P("section", "dp", None),
            P("section", "dp", None),
            P("section", None, None),
            P("section", None, None),
            P(None, "section"),
            P("section", None),
            P(),
            P(),
            P(),
        ),
        out_specs=(P("dp", None), P("dp", "section"), P(("section", "dp"), None)),
        check_vma=False,
    )
```

```python
import functools
import math

import jax
import jax.numpy as jnp
import numpy as np
from jax import lax
from jax.experimental import pallas as pl
from jax.experimental.pallas import tpu as pltpu
from jax.sharding import PartitionSpec as P

CH = 16
TSTEPS = 1000
STRIDE = 125


norm_eps = 1e-06


def shifted(shard, axis, by):
    length = lax.axis_size(axis)
    return lax.ppermute(shard, axis, [(i, (i + by) % length) for i in range(length)])


def from_root(shard, axis, root):
    mine = lax.axis_index(axis) == root
    return lax.psum(jnp.where(mine, shard, jnp.zeros_like(shard)), axis)


def layer_norm(values):
    center = values - jnp.mean(values, axis=-1, keepdims=True)
    spread = jnp.mean(center * center, axis=-1, keepdims=True)
    return center * lax.rsqrt(spread + norm_eps)


def sinusoid(step_ids, model_width):
    half_width = model_width // 2
    frequency = jnp.exp(-math.log(10000.0) * jnp.arange(half_width, dtype=jnp.float32) / half_width)
    phase_arg = step_ids.astype(jnp.float32)[:, None] * frequency[None, :]
    return jnp.concatenate([jnp.cos(phase_arg), jnp.sin(phase_arg)], axis=-1)


def plan(step_ids):
    angle_t = 0.5 * math.pi / TSTEPS * step_ids.astype(jnp.float32)
    return (jnp.cos(angle_t), jnp.sin(angle_t))


def embed_tokens(latent, embed_in):
    leading = latent.shape[0]
    patches = latent.reshape(leading * (latent.shape[1] // CH), CH).astype(jnp.bfloat16)
    tokens = jnp.dot(patches, embed_in, preferred_element_type=jnp.float32)
    return tokens.reshape(leading, latent.shape[1] // CH, embed_in.shape[1]).astype(jnp.bfloat16)


def mlp_block(inputs, modulation, up_proj, down_proj):
    groups, seq_len, model_width = inputs.shape
    residual_in = inputs.astype(jnp.float32)
    shift_rows = modulation[:, 0, None, :]
    scale_rows = modulation[:, 1, None, :]
    gate_rows = modulation[:, 2, None, :]
    normed = (layer_norm(residual_in) * (1.0 + scale_rows) + shift_rows).astype(jnp.bfloat16)
    pre_act = jnp.dot(
        normed.reshape(groups * seq_len, model_width), up_proj, preferred_element_type=jnp.float32
    )
    hidden = jax.nn.gelu(pre_act, approximate=True).astype(jnp.bfloat16)
    mixed = jnp.dot(hidden, down_proj, preferred_element_type=jnp.float32).reshape(
        groups, seq_len, model_width
    )
    return (residual_in + gate_rows * mixed).astype(jnp.bfloat16)


def velocity(states, embed_out):
    groups, seq_len, model_width = states.shape
    normed = layer_norm(states.astype(jnp.float32)).astype(jnp.bfloat16)
    result = jnp.dot(
        normed.reshape(groups * seq_len, model_width), embed_out, preferred_element_type=jnp.float32
    )
    return result.reshape(groups, seq_len * embed_out.shape[1])


def ddim_step(latent, predicted, time_now, time_next):
    alpha_now, sigma_now = plan(time_now)
    alpha_next, sigma_next = plan(time_next)
    clean_est = alpha_now[:, None] * latent - sigma_now[:, None] * predicted
    noise_est = sigma_now[:, None] * latent + alpha_now[:, None] * predicted
    return alpha_next[:, None] * clean_est + sigma_next[:, None] * noise_est


def gelu_slope(pre_act):
    return jax.vjp(lambda inner: jax.nn.gelu(inner, approximate=True), pre_act)[1](
        jnp.ones_like(pre_act)
    )[0]


def run_chunks(count, one, operands, shared):
    if count == 1:
        return one(operands, *shared)

    def step(carry, piece):
        out = one(piece, *shared)
        return (carry[0] + out[0], carry[1] + out[1]), None

    split = [a.reshape((count, a.shape[0] // count) + a.shape[1:]) for a in operands]
    shapes = jax.eval_shape(one, [a[0] for a in split], *shared)
    zeros = tuple(jnp.zeros(s.shape, s.dtype) for s in shapes)
    return lax.scan(step, zeros, split)[0]


def teacher_chain(first_in, noised, guidance, step_index, mods, up, down, embed_in, embed_out):
    section_count = lax.axis_size("section")
    section_at = lax.axis_index("section")
    micro, seq_len, model_width = first_in.shape

    def paired(tokens):
        return jnp.broadcast_to(tokens[:, None], (micro, 2, seq_len, model_width)).reshape(
            2 * micro, seq_len, model_width
        )

    latent = noised
    states = paired(first_in)
    for which_step in range(2):
        mod = mods[which_step].reshape(2 * micro, 3, model_width)
        if which_step:
            states = paired(embed_tokens(latent, embed_in))
        for layer in range(section_count):
            states = mlp_block(states, mod, up, down)
            if layer < section_count - 1:
                states = lax.ppermute(states, "section", [(layer, layer + 1)])
        predicted = velocity(states, embed_out).reshape(micro, 2, -1)
        weight = guidance[:, None]
        guided = (1.0 + weight) * predicted[:, 0] - weight * predicted[:, 1]
        time_now = step_index - which_step * STRIDE
        stepped = ddim_step(latent, guided, time_now, time_now - STRIDE)
        if which_step == 0:
            returned = lax.ppermute(
                stepped, "section", [(section_count - 1, 0)]
            )
            latent = jnp.where(section_at == section_count - 1, stepped, returned)
    return stepped


def cos_of(angle, shift_quarter):
    quarters = jnp.floor(angle * (2.0 / math.pi) + 0.5)
    rest = ((angle - quarters * 1.5703125) - quarters * 4.837512969970703125e-4) - (
        quarters * 7.549789954891882e-8
    )
    turn = quarters - shift_quarter
    turn = turn - 4.0 * jnp.floor(turn * 0.25)
    square = rest * rest
    sine = rest + rest * square * (
        -1.6666654611e-1 + square * (8.3321608736e-3 - 1.9515295891e-4 * square)
    )
    cosine = (
        1.0
        - 0.5 * square
        + square
        * square
        * (4.166664568298827e-2 + square * (-1.388731625493765e-3 + 2.443315711809948e-5 * square))
    )
    odd = (turn == 1.0) | (turn == 3.0)
    negative = (turn == 1.0) | (turn == 2.0)
    value = jnp.where(odd, sine, cosine)
    return jnp.where(negative, -value, value)


NT = (((1,), (1,)), ((), ()))
GELU_A = math.sqrt(2.0 / math.pi)
GELU_B = 0.044715


def dot32(a, b, dims=(((1,), (0,)), ((), ()))):
    return lax.dot_general(a, b, dims, preferred_element_type=jnp.float32)


def gelu_pair(pre):
    square = pre * pre
    bent = jnp.tanh(GELU_A * (pre + GELU_B * square * pre))
    half = 0.5 * (1.0 + bent)
    slope = half + 0.5 * pre * (1.0 - bent * bent) * (GELU_A * (1.0 + 3.0 * GELU_B * square))
    return pre * half, slope


def token_mask(first, count, shape):
    lane = lax.broadcasted_iota(jnp.int32, shape, 1) // CH
    return [lane == first + k for k in range(count)]


def spread(values, first, count):
    masks = token_mask(first, count, values.shape)
    zero = jnp.zeros_like(values)
    return jnp.concatenate([jnp.where(m, values, zero) for m in masks], axis=0)


def gathered_tokens(values, first, count, rows):
    masks = token_mask(first, count, (rows, values.shape[1]))
    total = jnp.zeros((rows, values.shape[1]), jnp.float32)
    for k in range(count):
        total = total + jnp.where(masks[k], values[k * rows : (k + 1) * rows], 0.0)
    return total


def mega_kernel(
    dims,
    steps_hbm, labels_hbm, levels_hbm, clean_in, noise_in, up_shard, down_shard,
    *rest_refs,
):
    small_hbm, rest_refs = rest_refs[:8], rest_refs[8:]
    stud_up_hbm, stud_down_hbm, table_hbm, target_out, grad_up, grad_down = rest_refs[:6]
    steps_in, labels_in, levels_in = rest_refs[6:9]
    small, rest_refs = rest_refs[9:17], rest_refs[17:]
    t_gain, t_bias, s_gain, s_bias, guide_vec, freq, embed_in, embed_out_t = small
    (
    stud_up, stud_down, table, packed, up, down, tiled_in, tiled_out,
    noised, cols, wave, labs, scond, tok, slope, n_share, h_share, parts, pair_in, pair_sum,
    cross_in, mixed, xhat, rstd, pred, states, outs, latents, velo, target_all, hid,
    local_sem, send, recv, move_send, move_recv, z_send, z_recv, t_send, t_recv, near,
    ) = rest_refs
    sections, dps, micro, seq_len = dims
    total = dps * micro
    width = clean_in.shape[1]
    model = embed_in.shape[1]
    sec = lax.axis_index("section")
    me = lax.axis_index("dp")
    z, y = me // 2, me % 2
    core, side = sec % 2, z // 2
    tail = sections - 1
    mid_z, end_z, far_mid_z = 1 + side, 3 * side, 2 - side
    far_end_z = 3 - end_z
    is_mid = z == mid_z
    is_end = z == end_z
    oy = 1 - y
    E_y, E_o = end_z * 2 + y, end_z * 2 + oy
    A_y, A_o = mid_z * 2 + y, mid_z * 2 + oy
    B_y, B_o = far_mid_z * 2 + y, far_mid_z * 2 + oy
    F_y, F_o = far_end_z * 2 + y, far_end_z * 2 + oy
    MESH = pl.DeviceIdType.MESH
    devices = sections * dps
    mine = sec * dps + me

    barrier = pltpu.get_barrier_semaphore()

    peer_y = z * 2 + oy

    def hello(semaphore, **device):
        pl.semaphore_signal(semaphore, inc=1, device_id=device, device_id_type=MESH)

    sibling = sec + 1 - 2 * core
    opposite = lax.rem(sec + 2, sections)
    hello(barrier, dp=peer_y)
    hello(barrier, section=sibling)
    hello(barrier, section=opposite)

    @pl.when(is_mid)
    def _():
        hello(barrier, dp=E_y)
        hello(barrier, dp=B_y)

    @pl.when(is_end)
    def _():
        hello(barrier, dp=A_y)

    def place(who):
        zz, yy = who // 2, who % 2
        return (zz % 2) * (dps // 2) + (zz // 2) * 2 + yy

    slot = place(me)
    locals_ = [
        pltpu.make_async_copy(stud_up_hbm, stud_up, local_sem.at[0]),
        pltpu.make_async_copy(stud_down_hbm, stud_down, local_sem.at[1]),
        pltpu.make_async_copy(table_hbm, table, local_sem.at[2]),
    ]
    ur, dr = up_shard.shape[0], down_shard.shape[0]

    def urow(who):
        return up.at[pl.ds(pl.multiple_of(who * ur, 16), ur)]

    def drow(who, lo=0, n=None):
        return down.at[pl.ds(pl.multiple_of(who * dr + lo, 16), dr if n is None else n)]

    shards = [
        pltpu.make_async_copy(up_shard, urow(me), local_sem.at[3]),
        pltpu.make_async_copy(down_shard, drow(me), local_sem.at[4]),
    ]
    first = [
        pltpu.make_async_copy(src, dst, local_sem.at[5 + k])
        for k, (src, dst) in enumerate(
            (
                (steps_hbm, steps_in), (labels_hbm, labels_in), (levels_hbm, levels_in),
                (clean_in, packed.at[slot, :, pl.ds(0, width)]),
                (noise_in, packed.at[slot, :, pl.ds(width, width)]),
            )
        )
    ]
    later = [
        pltpu.make_async_copy(src, dst, local_sem.at[10 + k])
        for k, (src, dst) in enumerate(zip(small_hbm, small))
    ]
    for c in shards + later + locals_:
        c.start()

    @pl.when(core == 1)
    def _():
        for c in first:
            c.start()

    pl.semaphore_wait(barrier, 4 + jnp.where(is_mid, 1, 0))

    def copy(i, src, dst, **device):
        return pltpu.make_async_remote_copy(
            src_ref=src, dst_ref=dst, send_sem=send.at[i], recv_sem=recv.at[i],
            device_id=device, device_id_type=MESH,
        )

    packs = [
        copy(k - 1, packed.at[slot], packed.at[slot], dp=lax.rem(me + k, dps))
        for k in range(1, dps)
    ]
    base = dps - 1
    names = [
        "ey_u", "ey_d", "ez_u", "ez_d", "ezo_u", "ezo_d", "ezo_r", "det1", "det2", "det3",
        "ay_u", "ay_d", "am_u", "am_d", "ame_u", "ame_d", "amo",
        "ayf_u", "ayf_d", "aye_u", "aye_d", "pair", "cross", "back", "hand",
    ]
    index = {n: base + k for k, n in enumerate(names)}
    cut = (2 * dr // 3) // 16 * 16
    low, high = (0, cut), (cut, dr - cut)
    span = {"ezo_d": low, "ezo_r": high, "det1": low, "det2": low, "det3": low, "amo": low, "ay_d": high, "aye_d": high}

    def piece(name, who, dst):
        ref = urow(who) if name.endswith("u") else drow(who, *span.get(name, (0, dr)))
        return copy(index[name], ref, ref, dp=dst)

    hand = copy(index["hand"], packed, packed, section=sibling)
    end_sends = (("ez_u", A_y), ("ey_u", E_o), ("ez_d", A_y), ("ey_d", E_o))
    mid_sends = (
        ("am_u", B_y), ("ay_u", A_o), ("det1", E_y), ("am_d", B_y), ("ay_d", A_o)
    )

    def begin():
        @pl.when(is_end)
        def _():
            for n, dst in end_sends:
                piece(n, me, dst).start()

        @pl.when(is_mid)
        def _():
            for n, dst in mid_sends:
                piece(n, me, dst).start()

    def relay(part):
        @pl.when(is_end)
        def _():
            piece("ey_" + part, E_o, E_o).wait_recv()
            piece("ezo_" + part, E_o, A_y).start()
            if part == "d":
                piece("ezo_r", E_o, A_y).start()
            if part == "u":
                piece("det1", A_y, E_o).wait_recv()
                piece("det2", A_y, E_o).start()
            else:
                piece("det2", A_o, A_y).wait_recv()
                piece("det3", A_o, A_y).start()

        @pl.when(is_mid)
        def _():
            piece("ez_" + part, E_y, B_y).wait_recv()
            piece("ame_" + part, E_y, B_y).start()
            piece("am_" + part, B_y, A_o).wait_recv()
            piece("ayf_" + part, B_y, A_o).start()

    def third():
        @pl.when(is_mid)
        def _():
            piece("ame_u", F_y, A_o).wait_recv()
            piece("aye_u", F_y, A_o).start()

    def fourth():
        @pl.when(is_mid)
        def _():
            piece("ezo_d", E_o, B_y).wait_recv()
            piece("amo", E_o, B_y).start()
            piece("ame_d", F_y, A_o).wait_recv()
            piece("aye_d", F_y, A_o).start()

    for c in shards:
        c.wait()

    @pl.when(core == 0)
    def _():
        begin()

    @pl.when(is_mid)
    def _():
        hello(near.at[0], dp=B_y)
        pl.semaphore_wait(near.at[0], 1)
        hello(near.at[0], dp=E_y)

    @pl.when(is_end)
    def _():
        pl.semaphore_wait(near.at[0], 1)

    hello(near.at[1], dp=peer_y)
    pl.semaphore_wait(near.at[1], 1)

    @pl.when(core == 1)
    def _():
        for c in first:
            c.wait()
        row = lax.broadcasted_iota(jnp.int32, (micro, 128), 0)
        column = lax.broadcasted_iota(jnp.int32, (micro, 128), 1)
        cells = jnp.zeros((micro, 128), jnp.float32)
        for k, ref in enumerate((steps_in, labels_in, levels_in)):
            for b in range(micro):
                cells = jnp.where((row == b) & (column == k), ref[b].astype(jnp.float32), cells)
        packed[slot, :, 2 * width :] = cells
        for c in packs:
            c.start()

    hello(near.at[2], section=opposite)
    for c in later:
        c.wait()
    pl.semaphore_wait(near.at[2], 1)
    hello(near.at[3], section=sibling)
    pl.semaphore_wait(near.at[3], 1)
    for k in range(seq_len):
        tiled_in[k * CH : (k + 1) * CH] = embed_in[...]
        tiled_out[k * CH : (k + 1) * CH] = embed_out_t[...]
    lane_model = lax.broadcasted_iota(jnp.int32, (1, model), 1)
    sine_lane = jnp.where(lane_model >= model // 2, 1.0, 0.0)

    @pl.when(core == 1)
    def _():
        for c in packs:
            c.wait_recv()
        hand.start()

    @pl.when(core == 0)
    def _():
        hand.wait_recv()

    data = packed[...].reshape(total, packed.shape[2])
    steps = data[:, 2 * width : 2 * width + 1]
    label = data[:, 2 * width + 1 : 2 * width + 2]
    guide = 0.5 * data[:, 2 * width + 2 : 2 * width + 3]
    for k in range(3):
        angle = jnp.broadcast_to(
            (0.5 * math.pi / TSTEPS) * (steps - float(k * STRIDE)), (total, 128)
        )
        cols[2 * k] = cos_of(angle, 0.0)
        cols[2 * k + 1] = cos_of(angle, 1.0)
    cols[6] = jnp.broadcast_to(guide, (total, 128))
    alpha_t, sigma_t = cols[0][:, 0:1], cols[1][:, 0:1]
    clean = alpha_t * data[:, :width] + sigma_t * data[:, width : 2 * width]
    noised[...] = clean
    for k in range(2):
        wave[k] = cos_of((steps - float(k * STRIDE)) * freq[...], sine_lane)
    for c in locals_:
        c.wait()
    classes = table.shape[0] - 1
    whole = (classes // 16) * 16
    ids = lax.broadcasted_iota(jnp.int32, (total, whole), 1).astype(jnp.float32)
    rows = dot32(jnp.where(ids == label, 1.0, 0.0).astype(jnp.bfloat16), table[:whole])
    rest = table[whole:].astype(jnp.float32)
    for k in range(classes - whole):
        rows = rows + jnp.where(label == float(whole + k), rest[k : k + 1], 0.0)
    labs[0] = rows
    labs[1] = jnp.broadcast_to(rest[classes - whole : classes - whole + 1], (total, model))
    vector = jnp.concatenate([guide_vec[k : k + 1] for k in range(model // 128)], axis=1)
    scond[...] = wave[0] + rows + guide * vector

    block = seq_len // 2
    blocks = 4
    group = total // 2
    brows = block * group
    share = n_share.shape[0]
    pick = jnp.where(
        lax.broadcasted_iota(jnp.int32, (share, model), 1)
        == lax.broadcasted_iota(jnp.int32, (share, model), 0) + me * share,
        1.0, 0.0,
    ).astype(jnp.bfloat16)

    def at_block(i):
        return pl.ds(pl.multiple_of(i * brows, brows), brows)

    def members(i):
        return pl.ds(pl.multiple_of((i // 2) * group, group), group)

    def first_of(i):
        return lax.rem(i, 2) * block

    def student_part(i, k):
        return scond[members(i)] * s_gain[k : k + 1] + s_bias[k : k + 1]

    def front(i, carry):
        here = at_block(i)
        tokens = dot32(
            spread(noised[members(i)], first_of(i), block).astype(jnp.bfloat16), tiled_in[...]
        ).astype(jnp.bfloat16)
        tok[here] = tokens
        cube = layer_norm(tokens.astype(jnp.float32)).reshape(block, group, model)
        normed = (cube * (1.0 + student_part(i, 1))[None] + student_part(i, 0)[None]).astype(
            jnp.bfloat16
        )
        normed = normed.reshape(brows, model)
        n_share[:, here] = dot32(pick, normed, NT).astype(jnp.bfloat16)
        hidden, bend = gelu_pair(dot32(normed, stud_up[...]))
        hidden = hidden.astype(jnp.bfloat16)
        slope[here] = bend
        h_share[:, here] = dot32(pick, hidden, NT).astype(jnp.bfloat16)
        parts[here] = dot32(hidden, stud_down[...]).astype(jnp.bfloat16)
        return carry

    @pl.when(core == 1)
    def _():
        begin()

    lax.fori_loop(0, blocks // 2, front, 0)

    @pl.when(core == 0)
    def _():
        relay("u")


    lax.fori_loop(blocks // 2, blocks, front, 0)

    half_rows = seq_len * total // 2

    def half_of(ref, c):
        return ref.at[pl.ds(pl.multiple_of(c * half_rows, half_rows), half_rows)]

    pair = copy(index["pair"], half_of(parts, 1 - core), pair_in, section=sibling)
    cross = copy(index["cross"], pair_sum, cross_in, section=opposite)
    back = copy(index["back"], half_of(mixed, core), half_of(mixed, core), section=sibling)
    pair.start()

    @pl.when(core == 0)
    def _():
        relay("d")

    @pl.when(core == 1)
    def _():
        relay("u")

    pair.wait_recv()
    pair_sum[...] = (
        half_of(parts, core)[...].astype(jnp.float32) + pair_in[...].astype(jnp.float32)
    ).astype(jnp.bfloat16)
    cross.start()

    @pl.when(core == 0)
    def _():
        third()

    turned = model // 4

    def turn(i, carry):
        here = pl.ds(pl.multiple_of(i * turned, turned), turned)
        eye = jnp.where(
            lax.broadcasted_iota(jnp.int32, (turned, model), 1)
            == lax.broadcasted_iota(jnp.int32, (turned, model), 0) + i * turned,
            1.0, 0.0,
        ).astype(jnp.bfloat16)
        stud_up[here] = dot32(eye, stud_down[...], NT).astype(jnp.bfloat16)
        return carry

    lax.fori_loop(0, 4, turn, 0)

    @pl.when(core == 0)
    def _():
        fourth()

    @pl.when(core == 1)
    def _():
        relay("d")

    cross.wait_recv()
    mixed[pl.ds(pl.multiple_of(core * half_rows, half_rows), half_rows)] = (
        pair_sum[...].astype(jnp.float32) + cross_in[...].astype(jnp.float32)
    ).astype(jnp.bfloat16)
    back.start()

    @pl.when(core == 1)
    def _():
        third()

    back.wait_recv()
    pred[...] = jnp.zeros_like(pred)

    def middle(i, carry):
        here = at_block(i)
        state = tok[here].astype(jnp.float32).reshape(block, group, model) + student_part(i, 2)[
            None
        ] * mixed[here].astype(jnp.float32).reshape(block, group, model)
        state = state.reshape(brows, model)
        center = state - jnp.mean(state, axis=-1, keepdims=True)
        inverse = lax.rsqrt(jnp.mean(center * center, axis=-1, keepdims=True) + norm_eps)
        unit = center * inverse
        xhat[here] = unit
        rstd[here] = jnp.broadcast_to(inverse, (brows, 128))
        pred[members(i)] += gathered_tokens(
            dot32(unit.astype(jnp.bfloat16), tiled_out[...], NT), first_of(i), block, group
        )
        return carry

    lax.fori_loop(0, blocks // 2, middle, 0)

    lax.fori_loop(blocks // 2, blocks, middle, 0)

    @pl.when(core == 1)
    def _():
        fourth()


    trows = micro * seq_len
    chunk = 768 if up.shape[1] % 768 == 0 else up.shape[1]

    def owned(j):
        return j * (dps // 2) + (z - 1) * 2 + y

    def sample_rows(d):
        return pl.ds(pl.multiple_of(d * micro, micro), micro)

    def move(i):
        return pltpu.make_async_remote_copy(
            src_ref=outs.at[i], dst_ref=states.at[i],
            send_sem=move_send.at[i], recv_sem=move_recv.at[i],
            device_id={"section": lax.rem(sec + 1, sections)}, device_id_type=MESH,
        )

    def back_move(j):
        return pltpu.make_async_remote_copy(
            src_ref=latents.at[1, j], dst_ref=latents.at[1, j],
            send_sem=z_send.at[j], recv_sem=z_recv.at[j],
            device_id={"section": 0}, device_id_type=MESH,
        )

    def target_copy(k, j, d):
        other = lax.rem(mine + k, devices)
        return pltpu.make_async_remote_copy(
            src_ref=target_all.at[d], dst_ref=target_all.at[d],
            send_sem=t_send.at[j * devices + k], recv_sem=t_recv.at[d],
            device_id={"section": other // dps, "dp": lax.rem(other, dps)}, device_id_type=MESH,
        )

    @pl.when(is_mid)
    def _():
        for n, who in (("ay_u", A_o), ("ayf_u", B_o), ("ezo_u", E_o), ("aye_u", F_o)):
            piece(n, who, A_o).wait_recv()
        for j in range(2):
            latents[0, j] = noised[sample_rows(owned(j))]

        def task(i, carry):
            step, j, half = i // 4, lax.rem(i // 2, 2), lax.rem(i, 2)
            d = owned(j)
            here = sample_rows(d)

            @pl.when(sec == 0)
            def _():
                @pl.when((step == 1) & (half == 0))
                def _():
                    back_move(j).wait_recv()

                states[i] = dot32(
                    spread(latents[step, j], 0, seq_len).astype(jnp.bfloat16), tiled_in[...]
                ).astype(jnp.bfloat16)

            @pl.when(sec > 0)
            def _():
                move(i).wait_recv()

            cond = wave[step, here] + labs[half, here]
            residual = states[i].astype(jnp.float32)
            cube = layer_norm(residual).reshape(seq_len, micro, model)
            scale = cond * t_gain[1] + t_bias[1]
            shift = cond * t_gain[0] + t_bias[0]
            gate = cond * t_gain[2] + t_bias[2]
            normed = (cube * (1.0 + scale)[None] + shift[None]).astype(jnp.bfloat16)
            normed = normed.reshape(trows, model)
            for k in range(up.shape[1] // chunk):
                hid[:, k * chunk : (k + 1) * chunk] = jax.nn.gelu(
                    dot32(normed, up[:, k * chunk : (k + 1) * chunk]), approximate=True
                ).astype(jnp.bfloat16)

            @pl.when(i == 0)
            def _():
                for n, who in (
                    ("ay_d", A_o), ("det3", A_o), ("ayf_d", B_o), ("aye_d", F_o), ("amo", F_o),
                    ("ezo_r", E_o),
                ):
                    piece(n, who, A_o).wait_recv()

            acc = dot32(hid[...], down[...])
            out = residual.reshape(seq_len, micro, model) + gate[None] * acc.reshape(
                seq_len, micro, model
            )
            outs[i] = out.reshape(trows, model).astype(jnp.bfloat16)

            @pl.when(sec < tail)
            def _():
                move(i).start()

            @pl.when(sec == tail)
            def _():
                last = layer_norm(outs[i].astype(jnp.float32)).astype(jnp.bfloat16)
                velo[half] = gathered_tokens(
                    dot32(last, tiled_out[...], NT), 0, seq_len, micro
                )

                @pl.when(half == 1)
                def _():
                    level = cols[6, here][:, 0:1]
                    guided = (1.0 + level) * velo[0] - level * velo[1]
                    a_now = cols[2 * step, here][:, 0:1]
                    s_now = cols[2 * step + 1, here][:, 0:1]
                    a_next = cols[2 * step + 2, here][:, 0:1]
                    s_next = cols[2 * step + 3, here][:, 0:1]
                    before = latents[step, j]
                    after = a_next * (a_now * before - s_now * guided) + s_next * (
                        s_now * before + a_now * guided
                    )

                    @pl.when(step == 0)
                    def _():
                        latents[1, j] = after
                        back_move(j).start()

                    @pl.when(step == 1)
                    def _():
                        a_first, s_first = cols[0, here][:, 0:1], cols[1, here][:, 0:1]
                        ratio = s_next / s_first
                        target_all[d] = (after - ratio * latents[0, j]) / (a_next - ratio * a_first)

                        def tell(k, carry):
                            target_copy(k, j, d).start()
                            return carry

                        lax.fori_loop(1, devices, tell, 0)

            return carry

        lax.fori_loop(0, 8, task, 0)

    grad_up[...] = jnp.zeros_like(grad_up)
    grad_down[...] = jnp.zeros_like(grad_down)

    def finish(i, carry):
        here = at_block(i)
        slopes = dot32(
            spread(pred[members(i)], first_of(i), block).astype(jnp.bfloat16), tiled_out[...]
        ) + dot32(
            spread(noised[members(i)], first_of(i), block).astype(jnp.bfloat16), tiled_out[...]
        )
        unit = xhat[here]
        mean = jnp.mean(slopes, axis=-1, keepdims=True)
        along = jnp.mean(slopes * unit, axis=-1, keepdims=True)
        back_state = rstd[here][:, 0:1] * (slopes - mean - unit * along)
        back_part = (student_part(i, 2)[None] * back_state.reshape(block, group, model)).astype(
            jnp.bfloat16
        ).reshape(brows, model)
        grad_down[...] += dot32(h_share[:, here], back_part)
        back_pre = (dot32(back_part, stud_up[...]) * slope[here]).astype(jnp.bfloat16)
        grad_up[...] += dot32(n_share[:, here], back_pre)
        return carry

    for part in range(2):
        for k in range(dps // 2):
            d = part * (dps // 2) + k

            @pl.when(jnp.logical_not((sec == tail) & (z == 1 + k // 2) & (y == k % 2)))
            def _():
                target_copy(1, 0, d).wait_recv()

        these = pl.ds(part * group, group)
        alpha_h, sigma_h = cols[0, these][:, 0:1], cols[1, these][:, 0:1]
        weight = jnp.maximum(alpha_h * alpha_h / (sigma_h * sigma_h), 1.0)
        estimate = alpha_h * noised[these] - sigma_h * pred[these]
        goal = target_all[pl.ds(part * (dps // 2), dps // 2)].reshape(group, width)
        seed = (-2.0 / (total * width)) * (sigma_h * weight) * (estimate - goal)
        seed_hi = seed.astype(jnp.bfloat16).astype(jnp.float32)
        pred[these] = seed_hi
        noised[these] = seed - seed_hi
        lax.fori_loop(2 * part, 2 * part + 2, finish, 0)

    target_out[...] = target_all[slot]

    for c in (pair, cross, back):
        c.wait_send()

    @pl.when(core == 1)
    def _():
        for c in packs + [hand]:
            c.wait_send()

    @pl.when(is_end)
    def _():
        for n, dst in end_sends:
            piece(n, me, dst).wait_send()
        for n, who, dst in (
            ("ezo_u", E_o, A_y), ("ezo_d", E_o, A_y), ("ezo_r", E_o, A_y),
            ("det2", A_y, E_o), ("det3", A_o, A_y),
        ):
            piece(n, who, dst).wait_send()

    @pl.when(is_mid)
    def _():
        for n, dst in mid_sends:
            piece(n, me, dst).wait_send()
        for n, who, dst in (
            ("ame_u", E_y, B_y), ("ame_d", E_y, B_y), ("amo", E_o, B_y),
            ("ayf_u", B_y, A_o), ("ayf_d", B_y, A_o), ("aye_u", F_y, A_o), ("aye_d", F_y, A_o),
        ):
            piece(n, who, dst).wait_send()

        @pl.when(sec < tail)
        def _():
            def done(i, carry):
                move(i).wait_send()
                return carry

            lax.fori_loop(0, 8, done, 0)

        @pl.when(sec == tail)
        def _():
            for j in range(2):
                back_move(j).wait_send()

                def told(k, carry):
                    target_copy(k, j, owned(j)).wait_send()
                    return carry

                lax.fori_loop(1, devices, told, 0)


def flush_kernel(a, b, c, x, y, z):
    x[...] = a[...]
    y[...] = b[...]
    z[...] = c[...]


def mega_call(dims, operands):
    sections, dps, micro, seq_len = dims
    clean, up_shard, down_shard = operands[3], operands[5], operands[6]
    hidden, model = up_shard.shape[1], down_shard.shape[1]
    stud_up, stud_down, table = operands[-3:]
    width = clean.shape[1]
    total = dps * micro
    rows = total * seq_len
    trows = micro * seq_len
    share_up, share_down = model // dps, stud_down.shape[0] // dps
    f32, bf16 = jnp.float32, jnp.bfloat16
    vmem = pl.BlockSpec(memory_space=pltpu.VMEM)
    hbm = pl.BlockSpec(memory_space=pltpu.HBM)
    V, D = pltpu.VMEM, pltpu.SemaphoreType.DMA
    results = pl.pallas_call(
        functools.partial(mega_kernel, dims),
        out_shape=(
            jax.ShapeDtypeStruct((micro, width), f32),
            jax.ShapeDtypeStruct((share_up, stud_up.shape[1]), f32),
            jax.ShapeDtypeStruct((share_down, model), f32),
        ),
        in_specs=[hbm] * len(operands),
        out_specs=(vmem,) * 3,
        scratch_shapes=[
            *[pltpu.SMEM(a.shape, a.dtype) for a in operands[:3]],
            *[V(a.shape, a.dtype) for a in operands[7:15]],
            V(stud_up.shape, bf16), V(stud_down.shape, bf16), V(table.shape, bf16),
            V((dps, micro, 2 * width + 128), f32),
            V((up_shard.shape[0] * dps, hidden), bf16),
            V((down_shard.shape[0] * dps, model), bf16),
            V((width, model), bf16), V((width, model), bf16),
            V((total, width), f32), V((7, total, 128), f32),
            V((2, total, model), f32), V((2, total, model), f32), V((total, model), f32),
            V((rows, model), bf16), V((rows, model), f32),
            V((share_up, rows), bf16), V((share_down, rows), bf16),
            V((rows, model), bf16), V((rows // 2, model), bf16), V((rows // 2, model), bf16),
            V((rows // 2, model), bf16), V((rows, model), bf16),
            V((rows, model), f32), V((rows, 128), f32), V((total, width), f32),
            V((8, trows, model), bf16), V((8, trows, model), bf16),
            V((2, 2, micro, width), f32), V((2, micro, width), f32), V((dps, micro, width), f32),
            V((trows, hidden), bf16),
            D((18,)), D((40,)), D((40,)), D((8,)), D((8,)), D((2,)), D((2,)),
            D((2 * sections * dps,)), D((dps,)),
            pltpu.SemaphoreType.REGULAR((4,)),
        ],
        compiler_params=pltpu.CompilerParams(
            collective_id=0, has_side_effects=True, vmem_limit_bytes=63 << 20
        ),
    )(*operands)
    return pl.pallas_call(
        flush_kernel,
        out_shape=tuple(jax.ShapeDtypeStruct(r.shape, r.dtype) for r in results),
        in_specs=[vmem] * 3,
        out_specs=(vmem,) * 3,
    )(*results)


def body(
    clean_latent,
    noise_draw,
    step_index,
    labels,
    guide_level,
    class_table,
    embed_in,
    embed_out,
    teacher_up,
    teacher_down,
    teacher_gain,
    teacher_bias,
    student_up,
    student_down,
    student_gain,
    student_bias,
    guide_vec,
):
    section_count = lax.axis_size("section")
    dp_count = lax.axis_size("dp")
    section_at = lax.axis_index("section")
    dp_at = lax.axis_index("dp")
    micro = clean_latent.shape[0]
    width = clean_latent.shape[1]
    seq_len = width // CH
    model_width = class_table.shape[1]
    fused = (
        dp_count == 8
        and section_count == 4
        and micro == 8
        and seq_len % 4 == 0
        and width % 128 == 0
        and model_width % 128 == 0
        and teacher_up.shape[1] % 16 == 0
        and teacher_down.shape[1] % 16 == 0
        and student_up.shape[1] == student_down.shape[0] == model_width
    )
    if fused:
        half_width = model_width // 2
        frequency = np.exp(-math.log(10000.0) * np.arange(half_width) / half_width)
        frequency = np.tile(frequency, 2)[None].astype(np.float32)
        return mega_call(
            (section_count, dp_count, micro, seq_len),
            (
                step_index, labels, guide_level, clean_latent, noise_draw,
                teacher_up[0], teacher_down[0],
                teacher_gain.reshape(3, 1, model_width), teacher_bias.reshape(3, 1, model_width),
                student_gain, student_bias, guide_vec.reshape(model_width // 128, 128), jnp.asarray(frequency),
                embed_in, embed_out.T, student_up, student_down, class_table,
            ),
        )
    alpha_t, sigma_t = plan(step_index)
    noised = alpha_t[:, None] * clean_latent + sigma_t[:, None] * noise_draw
    guidance = 0.5 * guide_level.astype(jnp.float32)
    label_rows = jnp.take(class_table, labels, axis=0).astype(jnp.float32)
    null_row = class_table[class_table.shape[0] - 1].astype(jnp.float32)
    wave_rows = jnp.stack(
        [sinusoid(step_index - step_k * STRIDE, model_width) for step_k in range(2)]
    )
    conditions = jnp.stack(
        [wave_rows + label_rows[None], wave_rows + null_row[None, None, :]], axis=2
    )
    mods = (
        conditions[:, :, :, None, :] * teacher_gain[0][None, None, None]
        + teacher_bias[0][None, None, None]
    )
    first_in = embed_tokens(noised, embed_in)
    alpha_end, sigma_end = plan(step_index - 2 * STRIDE)
    sigma_ratio = sigma_end / sigma_t
    packed = jnp.concatenate(
        [
            noised,
            step_index.astype(jnp.float32)[:, None],
            labels.astype(jnp.float32)[:, None],
            guide_level.astype(jnp.float32)[:, None],
        ],
        axis=1,
    )
    def student_normed(noised, steps, labels, guidance):
        rows = noised.shape[0] * seq_len
        label_rows = jnp.take(class_table, labels, axis=0).astype(jnp.float32)
        cond = sinusoid(steps, model_width) + label_rows + guidance[:, None] * guide_vec[None, :]
        modulation = cond[:, None, :] * student_gain[None] + student_bias[None]
        residual_in = embed_tokens(noised, embed_in).astype(jnp.float32)
        normed = (
            (layer_norm(residual_in) * (1.0 + modulation[:, 1, None, :]) + modulation[:, 0, None, :])
            .astype(jnp.bfloat16)
            .reshape(rows, model_width)
        )
        return residual_in, modulation[:, 2, None, :], normed

    def student_front(noised, steps, labels, guidance, student_up):
        residual_in, gate_rows, normed = student_normed(noised, steps, labels, guidance)
        pre_act = jnp.dot(normed, student_up, preferred_element_type=jnp.float32)
        hidden = jax.nn.gelu(pre_act, approximate=True).astype(jnp.bfloat16)
        return residual_in, gate_rows, normed, pre_act, hidden

    total = micro * dp_count
    element_count = total * width
    up_share = model_width // dp_count
    down_share = student_down.shape[0] // dp_count

    goal_scale = 1.0 / (alpha_end - sigma_ratio * alpha_t)
    up = lax.all_gather(teacher_up[0], "dp", axis=0, tiled=True)
    down = lax.all_gather(teacher_down[0], "dp", axis=0, tiled=True)
    ending = teacher_chain(
        first_in, noised, guidance, step_index, mods, up, down, embed_in, embed_out
    )
    goal_latent = (ending - sigma_ratio[:, None] * noised) * goal_scale[:, None]
    packed = lax.all_gather(packed, "dp", axis=0, tiled=True)
    own = student_front(noised, step_index, labels, guidance, student_up)
    partial_value = jnp.dot(own[4], student_down, preferred_element_type=jnp.float32)
    mixed = lax.psum(partial_value.astype(jnp.bfloat16), "section")
    all_mixed = lax.all_gather(mixed, "dp", axis=0, tiled=True)
    gathered = lax.all_gather(goal_latent, ("section", "dp"), axis=0, tiled=True)
    all_target = gathered[total * (section_count - 1):]
    all_mixed = all_mixed.reshape(total, seq_len, model_width)
    all_noised = packed[:, :width]
    all_steps = packed[:, width].astype(jnp.int32)
    all_labels = packed[:, width + 1].astype(jnp.int32)
    all_guidance = 0.5 * packed[:, width + 2]
    distill_target = lax.dynamic_slice_in_dim(all_target, dp_at * micro, micro, 0)

    def student_grads(operands, student_up, student_down):
        noised, steps, labels, guidance, mixed, target = operands
        count = noised.shape[0]
        rows = count * seq_len
        residual_in, gate_rows, normed, pre_act, hidden = student_front(
            noised, steps, labels, guidance, student_up
        )
        state_rows = residual_in + gate_rows * mixed.astype(jnp.float32)
        alpha_t, sigma_t = plan(steps)
        normed_out, pullback = jax.vjp(layer_norm, state_rows)
        predicted = jnp.dot(
            normed_out.astype(jnp.bfloat16).reshape(rows, model_width),
            embed_out,
            preferred_element_type=jnp.float32,
        ).reshape(count, width)
        estimate = alpha_t[:, None] * noised - sigma_t[:, None] * predicted
        weight = jnp.maximum(alpha_t * alpha_t / (sigma_t * sigma_t), 1.0)
        slope_pred = -2.0 / element_count * (sigma_t * weight)[:, None] * (estimate - target)
        back_norm = jnp.dot(
            slope_pred.reshape(rows, CH),
            embed_out.astype(jnp.float32).T,
            precision=lax.Precision.HIGHEST,
        )
        back_state = pullback(back_norm.reshape(count, seq_len, model_width))[0]
        back_part = (gate_rows * back_state).astype(jnp.bfloat16).reshape(rows, model_width)
        back_hidden = lax.dot_general(
            back_part, student_down, (((1,), (1,)), ((), ())), preferred_element_type=jnp.float32
        )
        back_pre = (back_hidden * gelu_slope(pre_act)).astype(jnp.bfloat16)
        normed_share = lax.dynamic_slice_in_dim(normed, dp_at * up_share, up_share, 1)
        hidden_share = lax.dynamic_slice_in_dim(hidden, dp_at * down_share, down_share, 1)
        contract_rows = (((0,), (0,)), ((), ()))
        return (
            lax.dot_general(
                normed_share, back_pre, contract_rows, preferred_element_type=jnp.float32
            ),
            lax.dot_general(
                hidden_share, back_part, contract_rows, preferred_element_type=jnp.float32
            ),
        )

    operands = [all_noised, all_steps, all_labels, all_guidance, all_mixed, all_target]
    grad_up, grad_down = run_chunks(
        max(1, dp_count // 8), student_grads, operands, (student_up, student_down)
    )
    return (distill_target, grad_up, grad_down)


def solution(mesh):
    return jax.shard_map(
        body,
        mesh=mesh,
        in_specs=(
            P("dp", None),
            P("dp", None),
            P("dp"),
            P("dp"),
            P("dp"),
            P(),
            P(),
            P(),
            P("section", "dp", None),
            P("section", "dp", None),
            P("section", None, None),
            P("section", None, None),
            P(None, "section"),
            P("section", None),
            P(),
            P(),
            P(),
        ),
        out_specs=(P("dp", None), P("dp", "section"), P(("section", "dp"), None)),
        check_vma=False,
    )
```

```python
import functools
import math

import jax
import jax.numpy as jnp
import numpy as np
from jax import lax
from jax.experimental import pallas as pl
from jax.experimental.pallas import tpu as pltpu
from jax.sharding import PartitionSpec as P

CH = 16
TSTEPS = 1000
STRIDE = 125


norm_eps = 1e-06


def shifted(shard, axis, by):
    length = lax.axis_size(axis)
    return lax.ppermute(shard, axis, [(i, (i + by) % length) for i in range(length)])


def from_root(shard, axis, root):
    mine = lax.axis_index(axis) == root
    return lax.psum(jnp.where(mine, shard, jnp.zeros_like(shard)), axis)


def layer_norm(values):
    center = values - jnp.mean(values, axis=-1, keepdims=True)
    spread = jnp.mean(center * center, axis=-1, keepdims=True)
    return center * lax.rsqrt(spread + norm_eps)


def sinusoid(step_ids, model_width):
    half_width = model_width // 2
    frequency = jnp.exp(-math.log(10000.0) * jnp.arange(half_width, dtype=jnp.float32) / half_width)
    phase_arg = step_ids.astype(jnp.float32)[:, None] * frequency[None, :]
    return jnp.concatenate([jnp.cos(phase_arg), jnp.sin(phase_arg)], axis=-1)


def plan(step_ids):
    angle_t = 0.5 * math.pi / TSTEPS * step_ids.astype(jnp.float32)
    return (jnp.cos(angle_t), jnp.sin(angle_t))


def embed_tokens(latent, embed_in):
    leading = latent.shape[0]
    patches = latent.reshape(leading * (latent.shape[1] // CH), CH).astype(jnp.bfloat16)
    tokens = jnp.dot(patches, embed_in, preferred_element_type=jnp.float32)
    return tokens.reshape(leading, latent.shape[1] // CH, embed_in.shape[1]).astype(jnp.bfloat16)


def mlp_block(inputs, modulation, up_proj, down_proj):
    groups, seq_len, model_width = inputs.shape
    residual_in = inputs.astype(jnp.float32)
    shift_rows = modulation[:, 0, None, :]
    scale_rows = modulation[:, 1, None, :]
    gate_rows = modulation[:, 2, None, :]
    normed = (layer_norm(residual_in) * (1.0 + scale_rows) + shift_rows).astype(jnp.bfloat16)
    pre_act = jnp.dot(
        normed.reshape(groups * seq_len, model_width), up_proj, preferred_element_type=jnp.float32
    )
    hidden = jax.nn.gelu(pre_act, approximate=True).astype(jnp.bfloat16)
    mixed = jnp.dot(hidden, down_proj, preferred_element_type=jnp.float32).reshape(
        groups, seq_len, model_width
    )
    return (residual_in + gate_rows * mixed).astype(jnp.bfloat16)


def velocity(states, embed_out):
    groups, seq_len, model_width = states.shape
    normed = layer_norm(states.astype(jnp.float32)).astype(jnp.bfloat16)
    result = jnp.dot(
        normed.reshape(groups * seq_len, model_width), embed_out, preferred_element_type=jnp.float32
    )
    return result.reshape(groups, seq_len * embed_out.shape[1])


def ddim_step(latent, predicted, time_now, time_next):
    alpha_now, sigma_now = plan(time_now)
    alpha_next, sigma_next = plan(time_next)
    clean_est = alpha_now[:, None] * latent - sigma_now[:, None] * predicted
    noise_est = sigma_now[:, None] * latent + alpha_now[:, None] * predicted
    return alpha_next[:, None] * clean_est + sigma_next[:, None] * noise_est


def gelu_slope(pre_act):
    return jax.vjp(lambda inner: jax.nn.gelu(inner, approximate=True), pre_act)[1](
        jnp.ones_like(pre_act)
    )[0]


def run_chunks(count, one, operands, shared):
    if count == 1:
        return one(operands, *shared)

    def step(carry, piece):
        out = one(piece, *shared)
        return (carry[0] + out[0], carry[1] + out[1]), None

    split = [a.reshape((count, a.shape[0] // count) + a.shape[1:]) for a in operands]
    shapes = jax.eval_shape(one, [a[0] for a in split], *shared)
    zeros = tuple(jnp.zeros(s.shape, s.dtype) for s in shapes)
    return lax.scan(step, zeros, split)[0]


def teacher_chain(first_in, noised, guidance, step_index, mods, up, down, embed_in, embed_out):
    section_count = lax.axis_size("section")
    section_at = lax.axis_index("section")
    micro, seq_len, model_width = first_in.shape

    def paired(tokens):
        return jnp.broadcast_to(tokens[:, None], (micro, 2, seq_len, model_width)).reshape(
            2 * micro, seq_len, model_width
        )

    latent = noised
    states = paired(first_in)
    for which_step in range(2):
        mod = mods[which_step].reshape(2 * micro, 3, model_width)
        if which_step:
            states = paired(embed_tokens(latent, embed_in))
        for layer in range(section_count):
            states = mlp_block(states, mod, up, down)
            if layer < section_count - 1:
                states = lax.ppermute(states, "section", [(layer, layer + 1)])
        predicted = velocity(states, embed_out).reshape(micro, 2, -1)
        weight = guidance[:, None]
        guided = (1.0 + weight) * predicted[:, 0] - weight * predicted[:, 1]
        time_now = step_index - which_step * STRIDE
        stepped = ddim_step(latent, guided, time_now, time_now - STRIDE)
        if which_step == 0:
            returned = lax.ppermute(
                stepped, "section", [(section_count - 1, 0)]
            )
            latent = jnp.where(section_at == section_count - 1, stepped, returned)
    return stepped


def cos_of(angle, shift_quarter):
    quarters = jnp.floor(angle * (2.0 / math.pi) + 0.5)
    rest = ((angle - quarters * 1.5703125) - quarters * 4.837512969970703125e-4) - (
        quarters * 7.549789954891882e-8
    )
    turn = quarters - shift_quarter
    turn = turn - 4.0 * jnp.floor(turn * 0.25)
    square = rest * rest
    sine = rest + rest * square * (
        -1.6666654611e-1 + square * (8.3321608736e-3 - 1.9515295891e-4 * square)
    )
    cosine = (
        1.0
        - 0.5 * square
        + square
        * square
        * (4.166664568298827e-2 + square * (-1.388731625493765e-3 + 2.443315711809948e-5 * square))
    )
    odd = (turn == 1.0) | (turn == 3.0)
    negative = (turn == 1.0) | (turn == 2.0)
    value = jnp.where(odd, sine, cosine)
    return jnp.where(negative, -value, value)


NT = (((1,), (1,)), ((), ()))
GELU_A = math.sqrt(2.0 / math.pi)
GELU_B = 0.044715


def dot32(a, b, dims=(((1,), (0,)), ((), ()))):
    return lax.dot_general(a, b, dims, preferred_element_type=jnp.float32)


def gelu_pair(pre):
    square = pre * pre
    bent = jnp.tanh(GELU_A * (pre + GELU_B * square * pre))
    half = 0.5 * (1.0 + bent)
    slope = half + 0.5 * pre * (1.0 - bent * bent) * (GELU_A * (1.0 + 3.0 * GELU_B * square))
    return pre * half, slope


def token_mask(first, count, shape):
    lane = lax.broadcasted_iota(jnp.int32, shape, 1) // CH
    return [lane == first + k for k in range(count)]


def spread(values, first, count):
    masks = token_mask(first, count, values.shape)
    zero = jnp.zeros_like(values)
    return jnp.concatenate([jnp.where(m, values, zero) for m in masks], axis=0)


def gathered_tokens(values, first, count, rows):
    masks = token_mask(first, count, (rows, values.shape[1]))
    total = jnp.zeros((rows, values.shape[1]), jnp.float32)
    for k in range(count):
        total = total + jnp.where(masks[k], values[k * rows : (k + 1) * rows], 0.0)
    return total


def mega_kernel(
    dims,
    steps_hbm, labels_hbm, levels_hbm, clean_in, noise_in, up_shard, down_shard,
    *rest_refs,
):
    small_hbm, rest_refs = rest_refs[:8], rest_refs[8:]
    stud_up_hbm, stud_down_hbm, table_hbm, target_out, grad_up, grad_down = rest_refs[:6]
    steps_in, labels_in, levels_in = rest_refs[6:9]
    small, rest_refs = rest_refs[9:17], rest_refs[17:]
    t_gain, t_bias, s_gain, s_bias, guide_vec, freq, embed_in, embed_out_t = small
    (
    stud_up, stud_down, table, packed, up, down, tiled_in, tiled_out,
    noised, cols, wave, labs, scond, tok, slope, n_share, h_share, parts, pair_in, pair_sum,
    cross_in, mixed, xhat, rstd, pred, states, outs, latents, velo, target_all, hid,
    local_sem, send, recv, move_send, move_recv, z_send, z_recv, t_send, t_recv, near,
    ) = rest_refs
    sections, dps, micro, seq_len = dims
    total = dps * micro
    width = clean_in.shape[1]
    model = embed_in.shape[1]
    sec = lax.axis_index("section")
    me = lax.axis_index("dp")
    z, y = me // 2, me % 2
    core, side = sec % 2, z // 2
    tail = sections - 1
    mid_z, end_z, far_mid_z = 1 + side, 3 * side, 2 - side
    far_end_z = 3 - end_z
    is_mid = z == mid_z
    is_end = z == end_z
    oy = 1 - y
    E_y, E_o = end_z * 2 + y, end_z * 2 + oy
    A_y, A_o = mid_z * 2 + y, mid_z * 2 + oy
    B_y, B_o = far_mid_z * 2 + y, far_mid_z * 2 + oy
    F_y, F_o = far_end_z * 2 + y, far_end_z * 2 + oy
    MESH = pl.DeviceIdType.MESH
    devices = sections * dps
    mine = sec * dps + me

    barrier = pltpu.get_barrier_semaphore()

    peer_y = z * 2 + oy

    def hello(semaphore, **device):
        pl.semaphore_signal(semaphore, inc=1, device_id=device, device_id_type=MESH)

    sibling = sec + 1 - 2 * core
    opposite = lax.rem(sec + 2, sections)
    hello(barrier, dp=peer_y)
    hello(barrier, section=sibling)
    hello(barrier, section=opposite)

    @pl.when(is_mid)
    def _():
        hello(barrier, dp=E_y)
        hello(barrier, dp=B_y)

    @pl.when(is_end)
    def _():
        hello(barrier, dp=A_y)

    def place(who):
        zz, yy = who // 2, who % 2
        return (zz % 2) * (dps // 2) + (zz // 2) * 2 + yy

    slot = place(me)
    locals_ = [
        pltpu.make_async_copy(stud_up_hbm, stud_up, local_sem.at[0]),
        pltpu.make_async_copy(stud_down_hbm, stud_down, local_sem.at[1]),
        pltpu.make_async_copy(table_hbm, table, local_sem.at[2]),
    ]
    ur, dr = up_shard.shape[0], down_shard.shape[0]

    def urow(who):
        return up.at[pl.ds(pl.multiple_of(who * ur, 16), ur)]

    def drow(who, lo=0, n=None):
        return down.at[pl.ds(pl.multiple_of(who * dr + lo, 16), dr if n is None else n)]

    shards = [
        pltpu.make_async_copy(up_shard, urow(me), local_sem.at[3]),
        pltpu.make_async_copy(down_shard, drow(me), local_sem.at[4]),
    ]
    first = [
        pltpu.make_async_copy(src, dst, local_sem.at[5 + k])
        for k, (src, dst) in enumerate(
            (
                (steps_hbm, steps_in), (labels_hbm, labels_in), (levels_hbm, levels_in),
                (clean_in, packed.at[slot, :, pl.ds(0, width)]),
                (noise_in, packed.at[slot, :, pl.ds(width, width)]),
            )
        )
    ]
    later = [
        pltpu.make_async_copy(src, dst, local_sem.at[10 + k])
        for k, (src, dst) in enumerate(zip(small_hbm, small))
    ]
    for c in shards + later + locals_:
        c.start()

    @pl.when(core == 1)
    def _():
        for c in first:
            c.start()

    pl.semaphore_wait(barrier, 4 + jnp.where(is_mid, 1, 0))

    def copy(i, src, dst, **device):
        return pltpu.make_async_remote_copy(
            src_ref=src, dst_ref=dst, send_sem=send.at[i], recv_sem=recv.at[i],
            device_id=device, device_id_type=MESH,
        )

    packs = [
        copy(k - 1, packed.at[slot], packed.at[slot], dp=lax.rem(me + k, dps))
        for k in range(1, dps)
    ]
    base = dps - 1
    names = [
        "ey_u", "ey_d", "ez_u", "ez_d", "ezo_u", "ezo_d", "ezo_r", "det1", "det2", "det3",
        "ay_u", "ay_d", "am_u", "am_d", "ame_u", "ame_d", "amo",
        "ayf_u", "ayf_d", "aye_u", "aye_d", "pair", "cross", "back", "hand",
    ]
    index = {n: base + k for k, n in enumerate(names)}
    cut = (2 * dr // 3) // 16 * 16
    low, high = (0, cut), (cut, dr - cut)
    span = {"ezo_d": low, "ezo_r": high, "det1": low, "det2": low, "det3": low, "amo": low, "ay_d": high, "aye_d": high}

    def piece(name, who, dst):
        ref = urow(who) if name.endswith("u") else drow(who, *span.get(name, (0, dr)))
        return copy(index[name], ref, ref, dp=dst)

    hand = copy(index["hand"], packed, packed, section=sibling)
    end_sends = (("ez_u", A_y), ("ey_u", E_o), ("ez_d", A_y), ("ey_d", E_o))
    mid_sends = (
        ("am_u", B_y), ("ay_u", A_o), ("det1", E_y), ("am_d", B_y), ("ay_d", A_o)
    )

    def begin():
        @pl.when(is_end)
        def _():
            for n, dst in end_sends:
                piece(n, me, dst).start()

        @pl.when(is_mid)
        def _():
            for n, dst in mid_sends:
                piece(n, me, dst).start()

    def relay(part):
        @pl.when(is_end)
        def _():
            piece("ey_" + part, E_o, E_o).wait_recv()
            piece("ezo_" + part, E_o, A_y).start()
            if part == "d":
                piece("ezo_r", E_o, A_y).start()
            if part == "u":
                piece("det1", A_y, E_o).wait_recv()
                piece("det2", A_y, E_o).start()
            else:
                piece("det2", A_o, A_y).wait_recv()
                piece("det3", A_o, A_y).start()

        @pl.when(is_mid)
        def _():
            piece("ez_" + part, E_y, B_y).wait_recv()
            piece("ame_" + part, E_y, B_y).start()
            piece("am_" + part, B_y, A_o).wait_recv()
            piece("ayf_" + part, B_y, A_o).start()

    def third():
        @pl.when(is_mid)
        def _():
            piece("ame_u", F_y, A_o).wait_recv()
            piece("aye_u", F_y, A_o).start()

    def fourth():
        @pl.when(is_mid)
        def _():
            piece("ezo_d", E_o, B_y).wait_recv()
            piece("amo", E_o, B_y).start()
            piece("ame_d", F_y, A_o).wait_recv()
            piece("aye_d", F_y, A_o).start()

    for c in shards:
        c.wait()

    @pl.when(core == 0)
    def _():
        begin()

    @pl.when(is_mid)
    def _():
        hello(near.at[0], dp=B_y)
        pl.semaphore_wait(near.at[0], 1)
        hello(near.at[0], dp=E_y)

    @pl.when(is_end)
    def _():
        pl.semaphore_wait(near.at[0], 1)

    hello(near.at[1], dp=peer_y)
    pl.semaphore_wait(near.at[1], 1)

    @pl.when(core == 1)
    def _():
        for c in first:
            c.wait()
        row = lax.broadcasted_iota(jnp.int32, (micro, 128), 0)
        column = lax.broadcasted_iota(jnp.int32, (micro, 128), 1)
        cells = jnp.zeros((micro, 128), jnp.float32)
        for k, ref in enumerate((steps_in, labels_in, levels_in)):
            for b in range(micro):
                cells = jnp.where((row == b) & (column == k), ref[b].astype(jnp.float32), cells)
        packed[slot, :, 2 * width :] = cells
        for c in packs:
            c.start()

    hello(near.at[2], section=opposite)
    for c in later:
        c.wait()
    pl.semaphore_wait(near.at[2], 1)
    hello(near.at[3], section=sibling)
    pl.semaphore_wait(near.at[3], 1)
    for k in range(seq_len):
        tiled_in[k * CH : (k + 1) * CH] = embed_in[...]
        tiled_out[k * CH : (k + 1) * CH] = embed_out_t[...]
    lane_model = lax.broadcasted_iota(jnp.int32, (1, model), 1)
    sine_lane = jnp.where(lane_model >= model // 2, 1.0, 0.0)

    @pl.when(core == 1)
    def _():
        for c in packs:
            c.wait_recv()
        hand.start()

    @pl.when(core == 0)
    def _():
        hand.wait_recv()

    data = packed[...].reshape(total, packed.shape[2])
    steps = data[:, 2 * width : 2 * width + 1]
    label = data[:, 2 * width + 1 : 2 * width + 2]
    guide = 0.5 * data[:, 2 * width + 2 : 2 * width + 3]
    for k in range(3):
        angle = jnp.broadcast_to(
            (0.5 * math.pi / TSTEPS) * (steps - float(k * STRIDE)), (total, 128)
        )
        cols[2 * k] = cos_of(angle, 0.0)
        cols[2 * k + 1] = cos_of(angle, 1.0)
    cols[6] = jnp.broadcast_to(guide, (total, 128))
    alpha_t, sigma_t = cols[0][:, 0:1], cols[1][:, 0:1]
    clean = alpha_t * data[:, :width] + sigma_t * data[:, width : 2 * width]
    noised[...] = clean
    for k in range(2):
        wave[k] = cos_of((steps - float(k * STRIDE)) * freq[...], sine_lane)
    for c in locals_:
        c.wait()
    classes = table.shape[0] - 1
    whole = (classes // 16) * 16
    ids = lax.broadcasted_iota(jnp.int32, (total, whole), 1).astype(jnp.float32)
    rows = dot32(jnp.where(ids == label, 1.0, 0.0).astype(jnp.bfloat16), table[:whole])
    rest = table[whole:].astype(jnp.float32)
    for k in range(classes - whole):
        rows = rows + jnp.where(label == float(whole + k), rest[k : k + 1], 0.0)
    labs[0] = rows
    labs[1] = jnp.broadcast_to(rest[classes - whole : classes - whole + 1], (total, model))
    vector = jnp.concatenate([guide_vec[k : k + 1] for k in range(model // 128)], axis=1)
    scond[...] = wave[0] + rows + guide * vector

    block = seq_len
    blocks = 2
    group = total // 2
    brows = block * group
    share = n_share.shape[0]
    pick = jnp.where(
        lax.broadcasted_iota(jnp.int32, (share, model), 1)
        == lax.broadcasted_iota(jnp.int32, (share, model), 0) + me * share,
        1.0, 0.0,
    ).astype(jnp.bfloat16)

    def at_block(i):
        return pl.ds(pl.multiple_of(i * brows, brows), brows)

    def members(i):
        return pl.ds(pl.multiple_of(i * group, group), group)

    def first_of(i):
        return 0

    def student_part(i, k):
        return scond[members(i)] * s_gain[k : k + 1] + s_bias[k : k + 1]

    def front(i, carry):
        here = at_block(i)
        tokens = dot32(
            spread(noised[members(i)], first_of(i), block).astype(jnp.bfloat16), tiled_in[...]
        ).astype(jnp.bfloat16)
        tok[here] = tokens
        cube = layer_norm(tokens.astype(jnp.float32)).reshape(block, group, model)
        normed = (cube * (1.0 + student_part(i, 1))[None] + student_part(i, 0)[None]).astype(
            jnp.bfloat16
        )
        normed = normed.reshape(brows, model)
        n_share[:, here] = dot32(pick, normed, NT).astype(jnp.bfloat16)
        hidden, bend = gelu_pair(dot32(normed, stud_up[...]))
        hidden = hidden.astype(jnp.bfloat16)
        slope[here] = bend
        h_share[:, here] = dot32(pick, hidden, NT).astype(jnp.bfloat16)
        parts[here] = dot32(hidden, stud_down[...]).astype(jnp.bfloat16)
        return carry

    @pl.when(core == 1)
    def _():
        begin()

    lax.fori_loop(0, blocks // 2, front, 0)

    @pl.when(core == 0)
    def _():
        relay("u")


    lax.fori_loop(blocks // 2, blocks, front, 0)

    half_rows = seq_len * total // 2

    def half_of(ref, c):
        return ref.at[pl.ds(pl.multiple_of(c * half_rows, half_rows), half_rows)]

    pair = copy(index["pair"], half_of(parts, 1 - core), pair_in, section=sibling)
    cross = copy(index["cross"], pair_sum, cross_in, section=opposite)
    back = copy(index["back"], half_of(mixed, core), half_of(mixed, core), section=sibling)
    pair.start()

    @pl.when(core == 0)
    def _():
        relay("d")

    @pl.when(core == 1)
    def _():
        relay("u")

    pair.wait_recv()
    pair_sum[...] = (
        half_of(parts, core)[...].astype(jnp.float32) + pair_in[...].astype(jnp.float32)
    ).astype(jnp.bfloat16)
    cross.start()

    @pl.when(core == 0)
    def _():
        third()

    turned = model // 4

    def turn(i, carry):
        here = pl.ds(pl.multiple_of(i * turned, turned), turned)
        eye = jnp.where(
            lax.broadcasted_iota(jnp.int32, (turned, model), 1)
            == lax.broadcasted_iota(jnp.int32, (turned, model), 0) + i * turned,
            1.0, 0.0,
        ).astype(jnp.bfloat16)
        stud_up[here] = dot32(eye, stud_down[...], NT).astype(jnp.bfloat16)
        return carry

    lax.fori_loop(0, 4, turn, 0)

    @pl.when(core == 0)
    def _():
        fourth()

    @pl.when(core == 1)
    def _():
        relay("d")

    cross.wait_recv()
    mixed[pl.ds(pl.multiple_of(core * half_rows, half_rows), half_rows)] = (
        pair_sum[...].astype(jnp.float32) + cross_in[...].astype(jnp.float32)
    ).astype(jnp.bfloat16)
    back.start()

    @pl.when(core == 1)
    def _():
        third()

    back.wait_recv()
    pred[...] = jnp.zeros_like(pred)

    def middle(i, carry):
        here = at_block(i)
        state = tok[here].astype(jnp.float32).reshape(block, group, model) + student_part(i, 2)[
            None
        ] * mixed[here].astype(jnp.float32).reshape(block, group, model)
        state = state.reshape(brows, model)
        center = state - jnp.mean(state, axis=-1, keepdims=True)
        inverse = lax.rsqrt(jnp.mean(center * center, axis=-1, keepdims=True) + norm_eps)
        unit = center * inverse
        xhat[here] = unit
        rstd[here] = jnp.broadcast_to(inverse, (brows, 128))
        pred[members(i)] += gathered_tokens(
            dot32(unit.astype(jnp.bfloat16), tiled_out[...], NT), first_of(i), block, group
        )
        return carry

    lax.fori_loop(0, blocks // 2, middle, 0)

    lax.fori_loop(blocks // 2, blocks, middle, 0)

    @pl.when(core == 1)
    def _():
        fourth()


    trows = micro * seq_len
    chunk = up.shape[1]

    def owned(j):
        return j * (dps // 2) + (z - 1) * 2 + y

    def sample_rows(d):
        return pl.ds(pl.multiple_of(d * micro, micro), micro)

    def move(i):
        return pltpu.make_async_remote_copy(
            src_ref=outs.at[i], dst_ref=states.at[i],
            send_sem=move_send.at[i], recv_sem=move_recv.at[i],
            device_id={"section": lax.rem(sec + 1, sections)}, device_id_type=MESH,
        )

    def back_move(j):
        return pltpu.make_async_remote_copy(
            src_ref=latents.at[1, j], dst_ref=latents.at[1, j],
            send_sem=z_send.at[j], recv_sem=z_recv.at[j],
            device_id={"section": 0}, device_id_type=MESH,
        )

    def target_copy(k, j, d):
        other = lax.rem(mine + k, devices)
        return pltpu.make_async_remote_copy(
            src_ref=target_all.at[d], dst_ref=target_all.at[d],
            send_sem=t_send.at[j * devices + k], recv_sem=t_recv.at[d],
            device_id={"section": other // dps, "dp": lax.rem(other, dps)}, device_id_type=MESH,
        )

    @pl.when(is_mid)
    def _():
        for n, who in (("ay_u", A_o), ("ayf_u", B_o), ("ezo_u", E_o), ("aye_u", F_o)):
            piece(n, who, A_o).wait_recv()
        for j in range(2):
            latents[0, j] = noised[sample_rows(owned(j))]

        def task(i, carry):
            step, j, half = i // 4, lax.rem(i // 2, 2), lax.rem(i, 2)
            d = owned(j)
            here = sample_rows(d)

            @pl.when(sec == 0)
            def _():
                @pl.when((step == 1) & (half == 0))
                def _():
                    back_move(j).wait_recv()

                states[i] = dot32(
                    spread(latents[step, j], 0, seq_len).astype(jnp.bfloat16), tiled_in[...]
                ).astype(jnp.bfloat16)

            @pl.when(sec > 0)
            def _():
                move(i).wait_recv()

            cond = wave[step, here] + labs[half, here]
            residual = states[i].astype(jnp.float32)
            cube = layer_norm(residual).reshape(seq_len, micro, model)
            scale = cond * t_gain[1] + t_bias[1]
            shift = cond * t_gain[0] + t_bias[0]
            gate = cond * t_gain[2] + t_bias[2]
            normed = (cube * (1.0 + scale)[None] + shift[None]).astype(jnp.bfloat16)
            normed = normed.reshape(trows, model)
            for k in range(up.shape[1] // chunk):
                hid[:, k * chunk : (k + 1) * chunk] = jax.nn.gelu(
                    dot32(normed, up[:, k * chunk : (k + 1) * chunk]), approximate=True
                ).astype(jnp.bfloat16)

            @pl.when(i == 0)
            def _():
                for n, who in (
                    ("ay_d", A_o), ("det3", A_o), ("ayf_d", B_o), ("aye_d", F_o), ("amo", F_o),
                    ("ezo_r", E_o),
                ):
                    piece(n, who, A_o).wait_recv()

            acc = dot32(hid[...], down[...])
            out = residual.reshape(seq_len, micro, model) + gate[None] * acc.reshape(
                seq_len, micro, model
            )
            outs[i] = out.reshape(trows, model).astype(jnp.bfloat16)

            @pl.when(sec < tail)
            def _():
                move(i).start()

            @pl.when(sec == tail)
            def _():
                last = layer_norm(outs[i].astype(jnp.float32)).astype(jnp.bfloat16)
                velo[half] = gathered_tokens(
                    dot32(last, tiled_out[...], NT), 0, seq_len, micro
                )

                @pl.when(half == 1)
                def _():
                    level = cols[6, here][:, 0:1]
                    guided = (1.0 + level) * velo[0] - level * velo[1]
                    a_now = cols[2 * step, here][:, 0:1]
                    s_now = cols[2 * step + 1, here][:, 0:1]
                    a_next = cols[2 * step + 2, here][:, 0:1]
                    s_next = cols[2 * step + 3, here][:, 0:1]
                    before = latents[step, j]
                    after = a_next * (a_now * before - s_now * guided) + s_next * (
                        s_now * before + a_now * guided
                    )

                    @pl.when(step == 0)
                    def _():
                        latents[1, j] = after
                        back_move(j).start()

                    @pl.when(step == 1)
                    def _():
                        a_first, s_first = cols[0, here][:, 0:1], cols[1, here][:, 0:1]
                        ratio = s_next / s_first
                        target_all[d] = (after - ratio * latents[0, j]) / (a_next - ratio * a_first)

                        def tell(k, carry):
                            target_copy(k, j, d).start()
                            return carry

                        lax.fori_loop(1, devices, tell, 0)

            return carry

        lax.fori_loop(0, 8, task, 0)

    grad_up[...] = jnp.zeros_like(grad_up)
    grad_down[...] = jnp.zeros_like(grad_down)

    def finish(i, carry):
        here = at_block(i)
        slopes = dot32(
            spread(pred[members(i)], first_of(i), block).astype(jnp.bfloat16), tiled_out[...]
        ) + dot32(
            spread(noised[members(i)], first_of(i), block).astype(jnp.bfloat16), tiled_out[...]
        )
        unit = xhat[here]
        mean = jnp.mean(slopes, axis=-1, keepdims=True)
        along = jnp.mean(slopes * unit, axis=-1, keepdims=True)
        back_state = rstd[here][:, 0:1] * (slopes - mean - unit * along)
        back_part = (student_part(i, 2)[None] * back_state.reshape(block, group, model)).astype(
            jnp.bfloat16
        ).reshape(brows, model)
        grad_down[...] += dot32(h_share[:, here], back_part)
        back_pre = (dot32(back_part, stud_up[...]) * slope[here]).astype(jnp.bfloat16)
        grad_up[...] += dot32(n_share[:, here], back_pre)
        return carry

    for part in range(2):
        for k in range(dps // 2):
            d = part * (dps // 2) + k

            @pl.when(jnp.logical_not((sec == tail) & (z == 1 + k // 2) & (y == k % 2)))
            def _():
                target_copy(1, 0, d).wait_recv()

        these = pl.ds(part * group, group)
        alpha_h, sigma_h = cols[0, these][:, 0:1], cols[1, these][:, 0:1]
        weight = jnp.maximum(alpha_h * alpha_h / (sigma_h * sigma_h), 1.0)
        estimate = alpha_h * noised[these] - sigma_h * pred[these]
        goal = target_all[pl.ds(part * (dps // 2), dps // 2)].reshape(group, width)
        seed = (-2.0 / (total * width)) * (sigma_h * weight) * (estimate - goal)
        seed_hi = seed.astype(jnp.bfloat16).astype(jnp.float32)
        pred[these] = seed_hi
        noised[these] = seed - seed_hi
        lax.fori_loop(part, part + 1, finish, 0)

    target_out[...] = target_all[slot]

    for c in (pair, cross, back):
        c.wait_send()

    @pl.when(core == 1)
    def _():
        for c in packs + [hand]:
            c.wait_send()

    @pl.when(is_end)
    def _():
        for n, dst in end_sends:
            piece(n, me, dst).wait_send()
        for n, who, dst in (
            ("ezo_u", E_o, A_y), ("ezo_d", E_o, A_y), ("ezo_r", E_o, A_y),
            ("det2", A_y, E_o), ("det3", A_o, A_y),
        ):
            piece(n, who, dst).wait_send()

    @pl.when(is_mid)
    def _():
        for n, dst in mid_sends:
            piece(n, me, dst).wait_send()
        for n, who, dst in (
            ("ame_u", E_y, B_y), ("ame_d", E_y, B_y), ("amo", E_o, B_y),
            ("ayf_u", B_y, A_o), ("ayf_d", B_y, A_o), ("aye_u", F_y, A_o), ("aye_d", F_y, A_o),
        ):
            piece(n, who, dst).wait_send()

        @pl.when(sec < tail)
        def _():
            def done(i, carry):
                move(i).wait_send()
                return carry

            lax.fori_loop(0, 8, done, 0)

        @pl.when(sec == tail)
        def _():
            for j in range(2):
                back_move(j).wait_send()

                def told(k, carry):
                    target_copy(k, j, owned(j)).wait_send()
                    return carry

                lax.fori_loop(1, devices, told, 0)


def flush_kernel(a, b, c, x, y, z, u, v, w, sems):
    reads = [
        pltpu.make_async_copy(src, mid, sems.at[k])
        for k, (src, mid) in enumerate(((a, u), (b, v), (c, w)))
    ]
    writes = [
        pltpu.make_async_copy(mid, dst, sems.at[3 + k])
        for k, (mid, dst) in enumerate(((u, x), (v, y), (w, z)))
    ]
    for c in reads:
        c.start()
    for c, d in zip(reads, writes):
        c.wait()
        d.start()
    for d in writes:
        d.wait()


def mega_call(dims, operands):
    sections, dps, micro, seq_len = dims
    clean, up_shard, down_shard = operands[3], operands[5], operands[6]
    hidden, model = up_shard.shape[1], down_shard.shape[1]
    stud_up, stud_down, table = operands[-3:]
    width = clean.shape[1]
    total = dps * micro
    rows = total * seq_len
    trows = micro * seq_len
    share_up, share_down = model // dps, stud_down.shape[0] // dps
    f32, bf16 = jnp.float32, jnp.bfloat16
    vmem = pl.BlockSpec(memory_space=pltpu.VMEM)
    hbm = pl.BlockSpec(memory_space=pltpu.HBM)
    V, D = pltpu.VMEM, pltpu.SemaphoreType.DMA
    results = pl.pallas_call(
        functools.partial(mega_kernel, dims),
        out_shape=(
            jax.ShapeDtypeStruct((micro, width), f32),
            jax.ShapeDtypeStruct((share_up, stud_up.shape[1]), f32),
            jax.ShapeDtypeStruct((share_down, model), f32),
        ),
        in_specs=[hbm] * len(operands),
        out_specs=(vmem,) * 3,
        scratch_shapes=[
            *[pltpu.SMEM(a.shape, a.dtype) for a in operands[:3]],
            *[V(a.shape, a.dtype) for a in operands[7:15]],
            V(stud_up.shape, bf16), V(stud_down.shape, bf16), V(table.shape, bf16),
            V((dps, micro, 2 * width + 128), f32),
            V((up_shard.shape[0] * dps, hidden), bf16),
            V((down_shard.shape[0] * dps, model), bf16),
            V((width, model), bf16), V((width, model), bf16),
            V((total, width), f32), V((7, total, 128), f32),
            V((2, total, model), f32), V((2, total, model), f32), V((total, model), f32),
            V((rows, model), bf16), V((rows, model), f32),
            V((share_up, rows), bf16), V((share_down, rows), bf16),
            V((rows, model), bf16), V((rows // 2, model), bf16), V((rows // 2, model), bf16),
            V((rows // 2, model), bf16), V((rows, model), bf16),
            V((rows, model), f32), V((rows, 128), f32), V((total, width), f32),
            V((8, trows, model), bf16), V((8, trows, model), bf16),
            V((2, 2, micro, width), f32), V((2, micro, width), f32), V((dps, micro, width), f32),
            V((trows, hidden), bf16),
            D((18,)), D((40,)), D((40,)), D((8,)), D((8,)), D((2,)), D((2,)),
            D((2 * sections * dps,)), D((dps,)),
            pltpu.SemaphoreType.REGULAR((4,)),
        ],
        compiler_params=pltpu.CompilerParams(
            collective_id=0, has_side_effects=True, vmem_limit_bytes=63 << 20
        ),
    )(*operands)
    return pl.pallas_call(
        flush_kernel,
        out_shape=tuple(jax.ShapeDtypeStruct(r.shape, r.dtype) for r in results),
        in_specs=[hbm] * 3,
        out_specs=(hbm,) * 3,
        scratch_shapes=[V(r.shape, r.dtype) for r in results] + [D((6,))],
    )(*results)


def body(
    clean_latent,
    noise_draw,
    step_index,
    labels,
    guide_level,
    class_table,
    embed_in,
    embed_out,
    teacher_up,
    teacher_down,
    teacher_gain,
    teacher_bias,
    student_up,
    student_down,
    student_gain,
    student_bias,
    guide_vec,
):
    section_count = lax.axis_size("section")
    dp_count = lax.axis_size("dp")
    section_at = lax.axis_index("section")
    dp_at = lax.axis_index("dp")
    micro = clean_latent.shape[0]
    width = clean_latent.shape[1]
    seq_len = width // CH
    model_width = class_table.shape[1]
    fused = (
        dp_count == 8
        and section_count == 4
        and micro == 8
        and seq_len % 4 == 0
        and width % 128 == 0
        and model_width % 128 == 0
        and teacher_up.shape[1] % 16 == 0
        and teacher_down.shape[1] % 16 == 0
        and student_up.shape[1] == student_down.shape[0] == model_width
    )
    if fused:
        half_width = model_width // 2
        frequency = np.exp(-math.log(10000.0) * np.arange(half_width) / half_width)
        frequency = np.tile(frequency, 2)[None].astype(np.float32)
        return mega_call(
            (section_count, dp_count, micro, seq_len),
            (
                step_index, labels, guide_level, clean_latent, noise_draw,
                teacher_up[0], teacher_down[0],
                teacher_gain.reshape(3, 1, model_width), teacher_bias.reshape(3, 1, model_width),
                student_gain, student_bias, guide_vec.reshape(model_width // 128, 128), jnp.asarray(frequency),
                embed_in, embed_out.T, student_up, student_down, class_table,
            ),
        )
    alpha_t, sigma_t = plan(step_index)
    noised = alpha_t[:, None] * clean_latent + sigma_t[:, None] * noise_draw
    guidance = 0.5 * guide_level.astype(jnp.float32)
    label_rows = jnp.take(class_table, labels, axis=0).astype(jnp.float32)
    null_row = class_table[class_table.shape[0] - 1].astype(jnp.float32)
    wave_rows = jnp.stack(
        [sinusoid(step_index - step_k * STRIDE, model_width) for step_k in range(2)]
    )
    conditions = jnp.stack(
        [wave_rows + label_rows[None], wave_rows + null_row[None, None, :]], axis=2
    )
    mods = (
        conditions[:, :, :, None, :] * teacher_gain[0][None, None, None]
        + teacher_bias[0][None, None, None]
    )
    first_in = embed_tokens(noised, embed_in)
    alpha_end, sigma_end = plan(step_index - 2 * STRIDE)
    sigma_ratio = sigma_end / sigma_t
    packed = jnp.concatenate(
        [
            noised,
            step_index.astype(jnp.float32)[:, None],
            labels.astype(jnp.float32)[:, None],
            guide_level.astype(jnp.float32)[:, None],
        ],
        axis=1,
    )
    def student_normed(noised, steps, labels, guidance):
        rows = noised.shape[0] * seq_len
        label_rows = jnp.take(class_table, labels, axis=0).astype(jnp.float32)
        cond = sinusoid(steps, model_width) + label_rows + guidance[:, None] * guide_vec[None, :]
        modulation = cond[:, None, :] * student_gain[None] + student_bias[None]
        residual_in = embed_tokens(noised, embed_in).astype(jnp.float32)
        normed = (
            (layer_norm(residual_in) * (1.0 + modulation[:, 1, None, :]) + modulation[:, 0, None, :])
            .astype(jnp.bfloat16)
            .reshape(rows, model_width)
        )
        return residual_in, modulation[:, 2, None, :], normed

    def student_front(noised, steps, labels, guidance, student_up):
        residual_in, gate_rows, normed = student_normed(noised, steps, labels, guidance)
        pre_act = jnp.dot(normed, student_up, preferred_element_type=jnp.float32)
        hidden = jax.nn.gelu(pre_act, approximate=True).astype(jnp.bfloat16)
        return residual_in, gate_rows, normed, pre_act, hidden

    total = micro * dp_count
    element_count = total * width
    up_share = model_width // dp_count
    down_share = student_down.shape[0] // dp_count

    goal_scale = 1.0 / (alpha_end - sigma_ratio * alpha_t)
    up = lax.all_gather(teacher_up[0], "dp", axis=0, tiled=True)
    down = lax.all_gather(teacher_down[0], "dp", axis=0, tiled=True)
    ending = teacher_chain(
        first_in, noised, guidance, step_index, mods, up, down, embed_in, embed_out
    )
    goal_latent = (ending - sigma_ratio[:, None] * noised) * goal_scale[:, None]
    packed = lax.all_gather(packed, "dp", axis=0, tiled=True)
    own = student_front(noised, step_index, labels, guidance, student_up)
    partial_value = jnp.dot(own[4], student_down, preferred_element_type=jnp.float32)
    mixed = lax.psum(partial_value.astype(jnp.bfloat16), "section")
    all_mixed = lax.all_gather(mixed, "dp", axis=0, tiled=True)
    gathered = lax.all_gather(goal_latent, ("section", "dp"), axis=0, tiled=True)
    all_target = gathered[total * (section_count - 1):]
    all_mixed = all_mixed.reshape(total, seq_len, model_width)
    all_noised = packed[:, :width]
    all_steps = packed[:, width].astype(jnp.int32)
    all_labels = packed[:, width + 1].astype(jnp.int32)
    all_guidance = 0.5 * packed[:, width + 2]
    distill_target = lax.dynamic_slice_in_dim(all_target, dp_at * micro, micro, 0)

    def student_grads(operands, student_up, student_down):
        noised, steps, labels, guidance, mixed, target = operands
        count = noised.shape[0]
        rows = count * seq_len
        residual_in, gate_rows, normed, pre_act, hidden = student_front(
            noised, steps, labels, guidance, student_up
        )
        state_rows = residual_in + gate_rows * mixed.astype(jnp.float32)
        alpha_t, sigma_t = plan(steps)
        normed_out, pullback = jax.vjp(layer_norm, state_rows)
        predicted = jnp.dot(
            normed_out.astype(jnp.bfloat16).reshape(rows, model_width),
            embed_out,
            preferred_element_type=jnp.float32,
        ).reshape(count, width)
        estimate = alpha_t[:, None] * noised - sigma_t[:, None] * predicted
        weight = jnp.maximum(alpha_t * alpha_t / (sigma_t * sigma_t), 1.0)
        slope_pred = -2.0 / element_count * (sigma_t * weight)[:, None] * (estimate - target)
        back_norm = jnp.dot(
            slope_pred.reshape(rows, CH),
            embed_out.astype(jnp.float32).T,
            precision=lax.Precision.HIGHEST,
        )
        back_state = pullback(back_norm.reshape(count, seq_len, model_width))[0]
        back_part = (gate_rows * back_state).astype(jnp.bfloat16).reshape(rows, model_width)
        back_hidden = lax.dot_general(
            back_part, student_down, (((1,), (1,)), ((), ())), preferred_element_type=jnp.float32
        )
        back_pre = (back_hidden * gelu_slope(pre_act)).astype(jnp.bfloat16)
        normed_share = lax.dynamic_slice_in_dim(normed, dp_at * up_share, up_share, 1)
        hidden_share = lax.dynamic_slice_in_dim(hidden, dp_at * down_share, down_share, 1)
        contract_rows = (((0,), (0,)), ((), ()))
        return (
            lax.dot_general(
                normed_share, back_pre, contract_rows, preferred_element_type=jnp.float32
            ),
            lax.dot_general(
                hidden_share, back_part, contract_rows, preferred_element_type=jnp.float32
            ),
        )

    operands = [all_noised, all_steps, all_labels, all_guidance, all_mixed, all_target]
    grad_up, grad_down = run_chunks(
        max(1, dp_count // 8), student_grads, operands, (student_up, student_down)
    )
    return (distill_target, grad_up, grad_down)


def solution(mesh):
    return jax.shard_map(
        body,
        mesh=mesh,
        in_specs=(
            P("dp", None),
            P("dp", None),
            P("dp"),
            P("dp"),
            P("dp"),
            P(),
            P(),
            P(),
            P("section", "dp", None),
            P("section", "dp", None),
            P("section", None, None),
            P("section", None, None),
            P(None, "section"),
            P("section", None),
            P(),
            P(),
            P(),
        ),
        out_specs=(P("dp", None), P("dp", "section"), P(("section", "dp"), None)),
        check_vma=False,
    )
```
